32 devices in a mesh: tm: 4 (over y, x), height: 8 (over z, core).
Axes of the slice: x: 2, y: 2, z: 4, core: 2. Of those that a mesh axis runs over, the one named last changes fastest.
Arguments:
- latent: bfloat16 [192, 2560], P(('tm', 'height')), may hold values from -9 to 9
- in_weight: bfloat16 [432, 384], replicated, may hold values from -0.3125 to 0.3125
- in_bias: float32 [384], replicated, may hold values from -3 to 3
- norm_gain: float32 [384], replicated, may hold values from 0.25 to 1.75
- norm_bias: float32 [384], replicated, may hold values from -3 to 3
- conv_weight: bfloat16 [10368, 384], replicated, may hold values from -0.0625 to 0.0625
- conv_bias: float32 [384], replicated, may hold values from -3 to 3
Outputs:
- features: bfloat16 [8, 24, 160, 384], P('tm', 'height')
The draws below stay inside these ranges and needn't reach their ends.
All inputs are finite; a program needn't handle non-finite values.
Results may differ from the reference program's by a relative error of at most 0.0027.
Values may be sent and summed in bfloat16 or wider, within the bound.
No kernel may reach another device: no remote copies, remote signals or barrier semaphores. Data moves between devices by JAX's collectives and lax.ppermute only.
A program may use at most 128 MiB of HBM per device.

```python
import jax
import jax.numpy as jnp
from jax import lax

C_IN = 16
CH = 384
GROUPS = 32
COLS = 160
FT = 8
HT = 24


def draw_latent(key, part):
    row_total = FT * HT
    first_key = jax.random.fold_in(key, 11)
    position = jnp.arange(row_total, dtype=jnp.float32) / max(row_total - 1, 1)
    rising = jnp.exp(jnp.log(3.0) * position)[:, None]
    values = jnp.clip(jax.random.normal(first_key, (row_total, COLS * C_IN), jnp.float32), -3.0, 3.0)
    return (values * rising).astype(jnp.bfloat16)


def bell_draw(own_key, shape, width, limit, held_as=jnp.bfloat16):
    drawn = jax.random.normal(own_key, shape, jnp.float32) * width
    return jnp.minimum(jnp.maximum(drawn, -limit), limit).astype(held_as)


def setup_inputs(seed: int = 0) -> dict:
    seeds = jax.random.split(jax.random.key(seed), 8)
    return {
        "latent": draw_latent(jax.random.fold_in(seeds[7], 71), 0),
        "in_weight": bell_draw(seeds[1], (27 * C_IN, CH), (27 * C_IN) ** -0.5, 0.3125),
        "in_bias": bell_draw(seeds[2], (CH,), 0.5, 3.0, jnp.float32),
        "norm_gain": jnp.clip(1.0 + 0.15 * jax.random.normal(seeds[3], (CH,), jnp.float32), 0.25, 1.75),
        "norm_bias": bell_draw(seeds[4], (CH,), 0.5, 3.0, jnp.float32),
        "conv_weight": bell_draw(seeds[5], (27 * CH, CH), (27 * CH) ** -0.5, 0.0625),
        "conv_bias": bell_draw(seeds[6], (CH,), 0.5, 3.0, jnp.float32),
    }


def causal_conv(source, weights, channels):
    padded = jnp.pad(source, ((2, 0), (1, 1), (1, 1), (0, 0)))

    def one_frame(frame_index):
        window = lax.dynamic_slice_in_dim(padded, frame_index.astype(jnp.int32), 3, 0)
        running = jnp.zeros((HT * COLS, weights.shape[1]), jnp.float32)
        for tap_t in range(3):
            for tap_h in range(3):
                for tap_w in range(3):
                    sliced = window[tap_t, tap_h:tap_h + HT, tap_w:tap_w + COLS, :].reshape(HT * COLS, channels)
                    tap_index = (tap_t * 3 + tap_h) * 3 + tap_w
                    running = running + jnp.dot(sliced, weights[tap_index * channels:(tap_index + 1) * channels], preferred_element_type=jnp.float32)
        return running.reshape(HT, COLS, weights.shape[1])
    return lax.map(one_frame, jnp.arange(FT, dtype=jnp.int32))

def reference(latent, in_weight, in_bias, norm_gain, norm_bias, conv_weight, conv_bias):
    latent_grid = latent.reshape(FT, HT, COLS, C_IN)
    opened = causal_conv(latent_grid, in_weight, C_IN) + in_bias
    per_group = CH // GROUPS
    grouped = opened.reshape(FT, HT, COLS, GROUPS, per_group)
    entries = FT * HT * COLS * per_group
    group_mean = lax.optimization_barrier(jnp.sum(grouped, axis=(0, 1, 2, 4))) / entries
    group_var = lax.optimization_barrier(jnp.sum(grouped * grouped, axis=(0, 1, 2, 4))) / entries - group_mean * group_mean
    group_scale = lax.rsqrt(group_var + 1e-06)
    normed = ((grouped - group_mean[:, None]) * group_scale[:, None]).reshape(FT, HT, COLS, CH)
    activated = jax.nn.silu(normed * norm_gain + norm_bias).astype(jnp.bfloat16)
    second = causal_conv(activated, conv_weight, CH) + conv_bias
    return (opened + second).astype(jnp.bfloat16)
```

```python
import functools

import jax
import jax.numpy as jnp
from jax import lax
from jax.experimental import pallas as pl
from jax.experimental.pallas import tpu as pltpu
from jax.sharding import PartitionSpec as P

C_IN = 16
GROUPS = 32
COLS = 160
FR_DEV = 2
SEG = 16
LANES = 128
F32 = jnp.float32
BF16 = jnp.bfloat16


def band_kernel(w_ref, o_ref):
    o_ref[...] = jnp.zeros_like(o_ref)
    channels = w_ref.shape[1]
    for ab in range(9):
        for q in range(5):
            row = ab * LANES + q * C_IN
            o_ref[row : row + 3 * C_IN, q * channels : (q + 1) * channels] = w_ref[
                ab * 3 * C_IN : (ab + 1) * 3 * C_IN, :
            ]


def opened_kernel(rows, own_ref, other_ref, halo_ref, band_ref, bias_ref, o_ref, sum_ref, z_ref, zb_ref, p_ref):
    core = lax.rem(lax.axis_index("height"), 2)
    slots = 3 * rows
    per = COLS // SEG
    width = COLS * C_IN

    def spread(piece, frame, slot):
        base = pl.multiple_of((frame * slots + slot) * SEG, SEG)
        count = piece.shape[0]
        edge = jnp.zeros((count, LANES), F32)
        wide = jnp.concatenate([edge, piece.astype(F32), edge, edge], axis=1)
        for s in range(SEG):
            for half in range(2):
                start = LANES + s * per * C_IN - C_IN + half * 5 * C_IN
                lo = start // LANES * LANES
                window = wide[:, lo : lo + 2 * LANES]
                if start > lo:
                    window = pltpu.roll(window, 2 * LANES - (start - lo), 1)
                z_ref[half, pl.ds(base + s, count, stride=SEG), :] = window[:, :LANES]

    main = jnp.where(core == 0, rows, 0)
    edge_slot = jnp.where(core == 0, rows - 2, 2 * rows)
    for d in range(3):
        spread(own_ref[d], 2 * d + core, main)
        spread(other_ref[d], 2 * d + 1 - core, main)
        spread(halo_ref[0, d], 2 * d + 1 - core, edge_slot)
        spread(halo_ref[1, d], 2 * d + core, edge_slot)
    for half in range(2):
        zb_ref[half] = z_ref[half].astype(BF16)

    high = rows + 2
    block = 4 * high * SEG
    for half in range(2):
        for t in range(4):
            for a in range(3):
                for b in range(3):
                    row = ((t + a) * slots + b + rows - 2) * SEG
                    dst = half * block + t * high * SEG
                    ab = a * 3 + b
                    p_ref[dst : dst + high * SEG, ab * LANES : (ab + 1) * LANES] = zb_ref[
                        half, row : row + high * SEG, :
                    ]

    channels = bias_ref.shape[1]
    tiles = channels // LANES
    total = 5 * tiles
    sums = [jnp.zeros((8, LANES), F32) for _ in range(tiles)]
    squares = [jnp.zeros((8, LANES), F32) for _ in range(tiles)]
    for n in range(0, total, 2):
        size = min(2, total - n)
        out = jnp.dot(p_ref[...], band_ref[:, n * LANES : (n + size) * LANES], preferred_element_type=F32)
        for i in range(size):
            q, tile = (n + i) // tiles, (n + i) % tiles
            lanes = slice(tile * LANES, (tile + 1) * LANES)
            part = out[:, i * LANES : (i + 1) * LANES] + bias_ref[:, lanes]
            for half in range(2):
                rest = part[half * block : (half + 1) * block]
                o_ref[:, half * 5 + q, :, lanes] = rest.reshape(4 * high, SEG, LANES)
                for t in range(2, 4):
                    begin = (t * high + 1) * SEG
                    mine = rest[begin : begin + rows * SEG].reshape(-1, 8, LANES)
                    sums[tile] = sums[tile] + jnp.sum(mine, axis=0)
                    squares[tile] = squares[tile] + jnp.sum(mine * mine, axis=0)
    for tile in range(tiles):
        lanes = slice(tile * LANES, (tile + 1) * LANES)
        sum_ref[0:1, lanes] = jnp.sum(sums[tile], axis=0, keepdims=True)
        sum_ref[1:2, lanes] = jnp.sum(squares[tile], axis=0, keepdims=True)


def second_kernel(rows, entries, sum_ref, o_ref, w_ref, gain_ref, shift_ref, bias_ref, out_ref, a_ref, f_ref):
    channels = gain_ref.shape[1]
    per = COLS // SEG
    high = rows + 2
    height = lax.axis_index("height")
    frame = lax.axis_index("tm")
    group = channels // GROUPS
    left = jnp.floor((lax.broadcasted_iota(jnp.int32, (channels, channels), 0).astype(F32) + 0.5) / group)
    right = jnp.floor((lax.broadcasted_iota(jnp.int32, (channels, channels), 1).astype(F32) + 0.5) / group)
    same = jnp.where(left == right, 1.0, 0.0).astype(F32)
    totals = jnp.dot(
        jnp.concatenate([sum_ref[...], jnp.zeros((6, channels), F32)], axis=0),
        same,
        precision=lax.Precision.HIGHEST,
        preferred_element_type=F32,
    )
    mean = totals[0:1] / entries
    var = totals[1:2] / entries - mean * mean
    scale = lax.rsqrt(var + 1e-06) * gain_ref[...]
    half_scale = 0.5 * scale
    half_shift = 0.5 * (shift_ref[...] - mean * scale)

    def act(index, carry):
        t = index // high
        h = index - t * high
        row = height * rows - 1 + h
        inside = (frame * FR_DEV - 2 + t >= 0) & (row >= 0) & (row < rows * lax.axis_size("height"))
        u = o_ref[index].reshape(per * SEG, channels) * half_scale + half_shift
        y = u + u * jnp.tanh(u)
        y = jnp.where(inside, y, 0.0)
        a_ref[index, 1 : per + 1] = y.astype(BF16).reshape(per, SEG, channels)
        lane_row = lax.broadcasted_iota(jnp.int32, (SEG, channels), 0)
        before = jnp.where(lane_row == 0, 0.0, pltpu.roll(y[(per - 1) * SEG :], 1, 0))
        after = jnp.where(lane_row == SEG - 1, 0.0, pltpu.roll(y[:SEG], SEG - 1, 0))
        a_ref[index, 0] = before.astype(BF16)
        a_ref[index, per + 1] = after.astype(BF16)
        return carry

    lax.fori_loop(0, 4 * high, act, 0)

    for t in range(2):

        def patch(tap):
            a, b, c = tap // 9, tap // 3 % 3, tap % 3
            start = (t + a) * high + b
            return a_ref[start : start + rows, c : c + per].reshape(rows * per * SEG, channels)

        acc = jnp.zeros((rows * per * SEG, channels), F32)
        for tap in range(0, 27, 2):
            taps = range(tap, min(tap + 2, 27))
            lhs = jnp.concatenate([patch(x) for x in taps], axis=1) if len(taps) > 1 else patch(tap)
            rhs = w_ref[tap * channels : (taps[-1] + 1) * channels, :]
            acc = acc + jnp.dot(lhs, rhs, preferred_element_type=F32)
        acc = acc + bias_ref[...]
        for h in range(rows):
            index = (t + 2) * high + h + 1
            whole = acc[h * per * SEG : (h + 1) * per * SEG] + o_ref[index].reshape(per * SEG, channels)
            for k in range(per):
                for tile in range(channels // LANES):
                    lanes = slice(tile * LANES, (tile + 1) * LANES)
                    f_ref[tile, pl.ds(k, SEG, stride=per), :] = whole[k * SEG : (k + 1) * SEG, lanes]
            for tile in range(channels // LANES):
                out_ref[t, h, :, tile * LANES : (tile + 1) * LANES] = f_ref[tile].astype(BF16)


def pairwise_sum(x, axis):
    size = lax.axis_size(axis)
    if size & (size - 1):
        return lax.psum(x, axis)
    step = 1
    while step < size:
        x = x + lax.ppermute(x, axis, [(i, i ^ step) for i in range(size)])
        step *= 2
    return x


def shards(latent, in_weight, in_bias, norm_gain, norm_bias, conv_weight, conv_bias):
    frames = FR_DEV
    rows = latent.shape[0] // frames
    channels = conv_weight.shape[1]
    tm, height = lax.axis_size("tm"), lax.axis_size("height")
    half = height // 2
    core = lax.axis_index("height") % 2
    band = pl.pallas_call(
        band_kernel, out_shape=jax.ShapeDtypeStruct((9 * LANES, 5 * channels), BF16), name="band"
    )(in_weight)

    received = []
    for d in (2, 1, 0):
        route = [
            (i * height + p * half + m, (i + d) * height + 2 * m + p)
            for i in range(tm - d)
            for p in range(2)
            for m in range(half)
        ]
        received.append(lax.ppermute(latent, ("tm", "height"), route))
    own = jnp.stack(received)
    other = lax.ppermute(own, "height", [(i, i ^ 1) for i in range(height)])
    edge = lax.dynamic_slice_in_dim(jnp.stack([own, other]), core * (2 * rows - 2), 2, axis=2)
    swap = [(2 * m - 1, 2 * m) for m in range(1, half)] + [(2 * m, 2 * m - 1) for m in range(1, half)]
    halo = lax.ppermute(edge, "height", swap)

    per = COLS // SEG
    high = rows + 2
    slots = 3 * rows
    opened, sums = pl.pallas_call(
        functools.partial(opened_kernel, rows),
        out_shape=(
            jax.ShapeDtypeStruct((4 * high, per, SEG, channels), F32),
            jax.ShapeDtypeStruct((2, channels), F32),
        ),
        scratch_shapes=[
            pltpu.VMEM((2, 6 * slots * SEG, LANES), F32),
            pltpu.VMEM((2, 6 * slots * SEG, LANES), BF16),
            pltpu.VMEM((8 * high * SEG, 9 * LANES), BF16),
        ],
        compiler_params=pltpu.CompilerParams(vmem_limit_bytes=24 << 20),
        name="opened",
    )(own, other, halo, band, in_bias[None])
    for axis in ("height", "tm"):
        sums = pairwise_sum(sums, axis)
    entries = frames * tm * rows * height * COLS * (channels // GROUPS)
    return pl.pallas_call(
        functools.partial(second_kernel, rows, entries),
        out_shape=jax.ShapeDtypeStruct((frames, rows, COLS, channels), BF16),
        scratch_shapes=[
            pltpu.VMEM((4 * high, per + 2, SEG, channels), BF16),
            pltpu.VMEM((channels // LANES, COLS, LANES), F32),
        ],
        compiler_params=pltpu.CompilerParams(vmem_limit_bytes=32 << 20),
        name="second",
    )(sums, opened, conv_weight, norm_gain[None], norm_bias[None], conv_bias[None])


def solution(mesh):
    return jax.shard_map(
        shards,
        mesh=mesh,
        in_specs=(P(("tm", "height"), None), P(), P(), P(), P(), P(), P()),
        out_specs=P("tm", "height", None, None),
        check_vma=False,
    )
```

```python
import functools

import jax
import jax.numpy as jnp
from jax import lax
from jax.experimental import pallas as pl
from jax.experimental.pallas import tpu as pltpu
from jax.sharding import PartitionSpec as P

C_IN = 16
GROUPS = 32
COLS = 160
FR_DEV = 2
SEG = 16
LANES = 128
F32 = jnp.float32
BF16 = jnp.bfloat16


def band_kernel(w_ref, *refs):
    *vectors, o_ref, v_ref = refs
    for i, vector in enumerate(vectors):
        v_ref[i : i + 1, :] = vector[...].reshape(1, -1)
    o_ref[...] = jnp.zeros_like(o_ref)
    channels = w_ref.shape[1]
    depth = 3 * C_IN
    places = [(a, b, a, b) for a in range(3) for b in range(2)] + [(0, 2, 3, 0), (1, 2, 3, 1), (2, 2, 4, 0)]
    for a, b, group, side in places:
        for e in range(2):
            row = group * LANES + side * (LANES // 2) + e * C_IN
            tap = (a * 3 + b) * depth
            o_ref[row : row + depth, e * channels : (e + 1) * channels] = w_ref[tap : tap + depth, :]


def windows(e_ref, f_ref, pair, frames, high):
    (t0, t1), (h0, h1) = frames, high
    rows = slice(h0 * SEG, h1 * SEG)
    parts = [e_ref[pair, t0 + a : t1 + a, rows] for a in range(3)]
    parts.append(f_ref[pair, t0:t1, rows])
    parts.append(e_ref[pair, t0 + 2 : t1 + 2, (h0 + 2) * SEG : (h1 + 2) * SEG])
    size = (t1 - t0) * (h1 - h0) * SEG
    return jnp.concatenate([part.reshape(size, LANES) for part in parts], axis=1)


def fetch(sem, *pairs):
    copies = [pltpu.make_async_copy(source, target, sem.at[i]) for i, (source, target) in enumerate(pairs)]
    for copy in copies:
        copy.start()
    return copies


def stats_kernel(
    rows, own_ref, other_ref, halo_ref, band_hbm, v_hbm, e_hbm, f_hbm, sum_ref, z_ref, band_ref, v_ref, e_ref, f_ref, sem
):
    loads = fetch(sem.at[0], (band_hbm, band_ref), (v_hbm, v_ref))
    core = lax.rem(lax.axis_index("height"), 2)
    slots = 3 * rows
    per = COLS // SEG
    high = rows + 2

    for frame in range(6):
        for slot in (0, slots - 1):
            row = (frame * slots + slot) * SEG
            for half in range(2):
                z_ref[half, row : row + SEG, :] = jnp.zeros((SEG, LANES), F32)

    def spread(piece, frame, slot):
        base = pl.multiple_of((frame * slots + slot) * SEG, SEG)
        count = piece.shape[0]
        edge = jnp.zeros((count, LANES), F32)
        wide = jnp.concatenate([edge, piece.astype(F32), edge, edge], axis=1)
        for s in range(SEG):
            for half in range(2):
                start = LANES + s * per * C_IN - C_IN + half * 6 * C_IN
                lo = start // LANES * LANES
                window = wide[:, lo : lo + 2 * LANES]
                if start > lo:
                    window = pltpu.roll(window, 2 * LANES - (start - lo), 1)
                z_ref[half, pl.ds(base + s, count, stride=SEG), :] = window[:, :LANES]

    main = jnp.where(core == 0, rows, 0)
    edge_slot = jnp.where(core == 0, rows - 2, 2 * rows)
    for d in range(3):
        spread(own_ref[d], 2 * d + core, main)
        spread(other_ref[d], 2 * d + 1 - core, main)
        spread(halo_ref[0, d], 2 * d + 1 - core, edge_slot)
        spread(halo_ref[1, d], 2 * d + core, edge_slot)

    first = rows - 2
    span = rows + 4
    low_side = lax.broadcasted_iota(jnp.int32, (span * SEG, LANES), 1) < LANES // 2
    where = [(0, 0), (0, 2 * C_IN), (0, 4 * C_IN), (1, 0), (1, 2 * C_IN)]

    def turned(x, shift):
        return x if shift % LANES == 0 else pltpu.roll(x, shift % LANES, 1)

    for pair, (half, offset) in enumerate(where):
        upper = []
        for frame in range(6):
            x = z_ref[half, pl.ds((frame * slots + first) * SEG, (span + 1) * SEG), :]
            low, up = turned(x, -offset), turned(x, LANES // 2 - offset)
            e_ref[pair, frame] = jnp.where(low_side, low[: span * SEG], up[SEG:]).astype(BF16)
            if 0 < frame < 5:
                f_ref[pair, frame - 1] = jnp.where(
                    low_side[: high * SEG], upper, up[2 * SEG : span * SEG]
                ).astype(BF16)
            upper = low[2 * SEG : span * SEG]

    channels = v_ref.shape[1]
    sums = jnp.zeros((8, 2 * channels), F32)
    squares = jnp.zeros((8, 2 * channels), F32)
    stores = fetch(sem.at[1], (e_ref, e_hbm), (f_ref, f_hbm))
    for load in loads:
        load.wait()
    bias = jnp.concatenate([v_ref[0:1, :], v_ref[0:1, :]], axis=1)
    for pair in range(per // 2):
        out = jnp.dot(
            windows(e_ref, f_ref, pair, (2, 4), (1, 1 + rows)), band_ref[...], preferred_element_type=F32
        )
        out = (out + bias).reshape(-1, 8, 2 * channels)
        sums = sums + jnp.sum(out, axis=0)
        squares = squares + jnp.sum(out * out, axis=0)
    for i, part in enumerate((sums, squares)):
        whole = jnp.sum(part, axis=0, keepdims=True)
        whole = whole[:, :channels] + whole[:, channels:]
        sum_ref[:, 0, i * channels : (i + 1) * channels] = jnp.broadcast_to(whole, (sum_ref.shape[0], channels))
    for store in stores:
        store.wait()


def opened_kernel(rows, e_hbm, f_hbm, band_hbm, v_hbm, o_hbm, e_ref, f_ref, band_ref, v_ref, o_ref, sem):
    for load in fetch(sem.at[0], (e_hbm, e_ref), (f_hbm, f_ref), (band_hbm, band_ref), (v_hbm, v_ref)):
        load.wait()
    channels = v_ref.shape[1]
    high = rows + 2
    stores = []
    for first in (0, 2):
        here = pl.ds(first, 2)
        for pair in range(COLS // SEG // 2):
            lhs = windows(e_ref, f_ref, pair, (first, first + 2), (0, high))
            out = jnp.dot(lhs, band_ref[...], preferred_element_type=F32)
            for e in range(2):
                part = out[:, e * channels : (e + 1) * channels] + v_ref[0:1, :]
                o_ref[here, :, 2 * pair + e] = part.reshape(2, high, SEG, channels)
        stores += fetch(sem.at[1 + first // 2], (o_ref.at[here], o_hbm.at[here]))
    for store in stores:
        store.wait()


def second_kernel(
    rows, entries, sum_ref, o_hbm, w_hbm, v_hbm, out_hbm,
    a_ref, place_ref, main_ref, two_ref, one_ref, w_ref, o_ref, v_ref, out_ref, sem,
):
    channels = v_ref.shape[1]
    per = COLS // SEG
    high = rows + 2
    third = 3 * channels
    weights = [
        pltpu.make_async_copy(w_hbm.at[pl.ds(i * third, third)], w_ref.at[pl.ds(i * third, third)], sem.at[i])
        for i in range(9)
    ]
    loads = [pltpu.make_async_copy(o_hbm.at[t], o_ref.at[t], sem.at[9 + t]) for t in range(4)]
    small = pltpu.make_async_copy(v_hbm, v_ref, sem.at[13])
    for copy in (small, loads[0], *weights[:3], loads[1], *weights[3:6], loads[2], *weights[6:], loads[3]):
        copy.start()
    height = lax.axis_index("height")
    frame = lax.axis_index("tm")
    group = channels // GROUPS
    left = jnp.floor((lax.broadcasted_iota(jnp.int32, (channels, channels), 0).astype(F32) + 0.5) / group)
    right = jnp.floor((lax.broadcasted_iota(jnp.int32, (channels, channels), 1).astype(F32) + 0.5) / group)
    same = jnp.where(left == right, 1.0, 0.0).astype(F32)
    total = jnp.sum(sum_ref[:, 0, :], axis=0, keepdims=True)
    both = jnp.concatenate([total[:, :channels], total[:, channels:], jnp.zeros((6, channels), F32)], axis=0)
    totals = jnp.dot(both, same, precision=lax.Precision.HIGHEST, preferred_element_type=F32)
    mean = totals[0:1] / entries
    var = totals[1:2] / entries - mean * mean
    small.wait()
    scale = lax.rsqrt(var + 1e-06) * v_ref[1:2, :]
    half_scale = 0.5 * scale
    half_shift = 0.5 * (v_ref[2:3, :] - mean * scale)
    lane_row = lax.broadcasted_iota(jnp.int32, (SEG, channels), 0)

    def act(t):
        for h in range(high):
            row = height * rows - 1 + h
            inside = (frame * FR_DEV - 2 + t >= 0) & (row >= 0) & (row < rows * lax.axis_size("height"))
            u = o_ref[t, h].reshape(per * SEG, channels) * half_scale + half_shift
            y = u + u * jnp.tanh(u)
            y = jnp.where(inside, y, 0.0)
            a_ref[t, h, 1 : per + 1] = y.astype(BF16).reshape(per, SEG, channels)
            before = jnp.where(lane_row == 0, 0.0, pltpu.roll(y[(per - 1) * SEG :], 1, 0))
            after = jnp.where(lane_row == SEG - 1, 0.0, pltpu.roll(y[:SEG], SEG - 1, 0))
            a_ref[t, h, 0] = before.astype(BF16)
            a_ref[t, h, per + 1] = after.astype(BF16)

    wide = channels // (2 * LANES) * 2 * LANES

    def patch(frame, b, c, count):
        return a_ref[frame, b : b + rows, c : c + count].reshape(rows * count * SEG, channels)

    def tap(a, b, c, lanes):
        row = ((a * 3 + b) * 3 + c) * channels
        return w_ref[row : row + channels, lanes]

    def product(pairs):
        acc = None
        for i in range(0, len(pairs), 2):
            some = pairs[i : i + 2]
            lhs = jnp.concatenate([x() for x, _ in some], axis=1)
            rhs = jnp.concatenate([y() for _, y in some], axis=0)
            part = jnp.dot(lhs, rhs, preferred_element_type=F32)
            acc = part if acc is None else acc + part
        return acc

    def unit(t, a):
        low, rest = slice(0, wide), slice(wide, channels)
        f = t + a
        main = product([
            (functools.partial(patch, f, b, c, per), functools.partial(tap, a, b, c, low))
            for b in range(3) for c in range(3)
        ])
        two = product([
            (
                functools.partial(patch, f, b, 0, per + 1),
                lambda b=b: jnp.concatenate([tap(a, b, 0, rest), tap(a, b, 1, rest)], axis=1),
            )
            for b in range(3)
        ])
        one = product([
            (functools.partial(patch, f, b, 2, per), functools.partial(tap, a, b, 2, rest)) for b in range(3)
        ])
        return main, two, one

    totals_refs = (main_ref, two_ref, one_ref)

    def begin(t):
        for ref, part in zip(totals_refs, unit(t, 0)):
            ref[t] = part

    def add(t, a):
        for ref, part in zip(totals_refs, unit(t, a)):
            ref[t] += part

    def finish(t):
        main, two, one = (ref[t] for ref in totals_refs)
        two = two.reshape(rows, per + 1, SEG, 2 * LANES)
        size = rows * per * SEG
        one = one + two[:, :per, :, :LANES].reshape(size, LANES) + two[:, 1:, :, LANES:].reshape(size, LANES)
        for h in range(rows):
            base = h * per * SEG
            opened = o_ref[t + 2, h + 1].reshape(per * SEG, channels)
            for tile in range(channels // LANES):
                lanes = slice(tile * LANES, (tile + 1) * LANES)
                source = main[:, lanes] if tile * LANES < wide else one
                whole = source[base : base + per * SEG] + v_ref[3:4, lanes] + opened[:, lanes]
                for k in range(per):
                    place_ref[t, h, tile, pl.ds(k, SEG, stride=per), :] = whole[k * SEG : (k + 1) * SEG]
                out_ref[t, h, :, lanes] = place_ref[t, h, tile].astype(BF16)
        store = pltpu.make_async_copy(out_ref.at[t], out_hbm.at[t], sem.at[14 + t])
        store.start()
        return store

    def need(*copies):
        for copy in copies:
            copy.wait()

    need(loads[0])
    act(0)
    need(*weights[:3], loads[1])
    act(1)
    begin(0)
    need(*weights[3:6], loads[2])
    act(2)
    add(0, 1)
    begin(1)
    need(*weights[6:], loads[3])
    act(3)
    add(0, 2)
    add(1, 1)
    first = finish(0)
    add(1, 2)
    second = finish(1)
    need(first, second)


def second_part(rows, entries, sums, opened, weight, vectors):
    high, per, channels, frames = rows + 2, COLS // SEG, vectors.shape[1], FR_DEV
    vmem, hbm = pl.BlockSpec(memory_space=pltpu.VMEM), pl.BlockSpec(memory_space=pltpu.HBM)
    size = rows * per * SEG
    out_shape = (frames, rows, COLS, channels)
    return pl.pallas_call(
        functools.partial(second_kernel, rows, entries),
        out_shape=pltpu.HBM(out_shape, BF16),
        in_specs=[vmem, hbm, hbm, hbm],
        out_specs=hbm,
        scratch_shapes=[
            pltpu.VMEM((4, high, per + 2, SEG, channels), BF16),
            pltpu.VMEM((frames, rows, channels // LANES, COLS, LANES), F32),
            pltpu.VMEM((frames, size, channels // (2 * LANES) * 2 * LANES), F32),
            pltpu.VMEM((frames, size // per * (per + 1), 2 * LANES), F32),
            pltpu.VMEM((frames, size, LANES), F32),
            pltpu.VMEM(weight.shape, BF16),
            pltpu.VMEM(opened.shape, F32),
            pltpu.VMEM(vectors.shape, F32),
            pltpu.VMEM(out_shape, BF16),
            pltpu.SemaphoreType.DMA((16,)),
        ],
        compiler_params=pltpu.CompilerParams(vmem_limit_bytes=36 << 20),
        name="second",
    )(sums, opened, weight, vectors)


def shards(latent, in_weight, in_bias, norm_gain, norm_bias, conv_weight, conv_bias):
    frames = FR_DEV
    rows = latent.shape[0] // frames
    channels = conv_weight.shape[1]
    tm, height = lax.axis_size("tm"), lax.axis_size("height")
    half = height // 2
    core = lax.axis_index("height") % 2
    band, vectors = pl.pallas_call(
        band_kernel,
        out_shape=(
            jax.ShapeDtypeStruct((5 * LANES, 2 * channels), BF16),
            jax.ShapeDtypeStruct((4, channels), F32),
        ),
        name="band",
    )(in_weight, in_bias, norm_gain, norm_bias, conv_bias)

    received = []
    for d in (2, 1, 0):
        route = [
            (i * height + p * half + m, (i + d) * height + 2 * m + p)
            for i in range(tm - d)
            for p in range(2)
            for m in range(half)
        ]
        received.append(lax.ppermute(latent, ("tm", "height"), route))
    own = jnp.stack(received)
    other = lax.ppermute(own, "height", [(i, i ^ 1) for i in range(height)])
    edge = lax.dynamic_slice_in_dim(jnp.stack([own, other]), core * (2 * rows - 2), 2, axis=2)
    swap = [(2 * m - 1, 2 * m) for m in range(1, half)] + [(2 * m, 2 * m - 1) for m in range(1, half)]
    halo = lax.ppermute(edge, "height", swap)

    per = COLS // SEG
    high = rows + 2
    vmem, hbm = pl.BlockSpec(memory_space=pltpu.VMEM), pl.BlockSpec(memory_space=pltpu.HBM)

    def keep(x):
        return pltpu.with_memory_space_constraint(x, pltpu.HBM)

    band, vectors = keep(band), keep(vectors)
    wide_shape, deep_shape = (per // 2, 6, (rows + 4) * SEG, LANES), (per // 2, 4, high * SEG, LANES)
    wide, deep, sums = pl.pallas_call(
        functools.partial(stats_kernel, rows),
        out_shape=(
            pltpu.HBM(wide_shape, BF16),
            pltpu.HBM(deep_shape, BF16),
            jax.ShapeDtypeStruct((tm * height, 1, 2 * channels), F32),
        ),
        in_specs=[vmem, vmem, vmem, hbm, hbm],
        out_specs=(hbm, hbm, vmem),
        scratch_shapes=[
            pltpu.VMEM((2, 6 * 3 * rows * SEG, LANES), F32),
            pltpu.VMEM(band.shape, BF16),
            pltpu.VMEM(vectors.shape, F32),
            pltpu.VMEM(wide_shape, BF16),
            pltpu.VMEM(deep_shape, BF16),
            pltpu.SemaphoreType.DMA((2, 2)),
        ],
        compiler_params=pltpu.CompilerParams(vmem_limit_bytes=12 << 20),
        name="stats",
    )(own, other, halo, band, vectors)
    everyone = [list(range(tm * height))[::-1]]
    sums = lax.all_to_all(sums, ("tm", "height"), 0, 0, tiled=True, axis_index_groups=everyone)
    positions = 4 * high * per * SEG
    opened_shape = (4, high, per, SEG, channels)
    opened = pl.pallas_call(
        functools.partial(opened_kernel, rows),
        out_shape=pltpu.HBM(opened_shape, F32),
        in_specs=[hbm, hbm, hbm, hbm],
        out_specs=hbm,
        scratch_shapes=[
            pltpu.VMEM(wide_shape, BF16),
            pltpu.VMEM(deep_shape, BF16),
            pltpu.VMEM(band.shape, BF16),
            pltpu.VMEM(vectors.shape, F32),
            pltpu.VMEM(opened_shape, F32),
            pltpu.SemaphoreType.DMA((3, 4)),
        ],
        cost_estimate=pl.CostEstimate(
            flops=2 * positions * 5 * LANES * channels, transcendentals=0, bytes_accessed=4 * positions * channels
        ),
        compiler_params=pltpu.CompilerParams(vmem_limit_bytes=16 << 20),
        name="opened",
    )(keep(wide), keep(deep), band, vectors)
    entries = frames * tm * rows * height * COLS * (channels // GROUPS)
    return second_part(rows, entries, sums, keep(opened), keep(conv_weight), vectors)


def solution(mesh):
    return jax.shard_map(
        shards,
        mesh=mesh,
        in_specs=(P(("tm", "height"), None), P(), P(), P(), P(), P(), P()),
        out_specs=P("tm", "height", None, None),
        check_vma=False,
    )
```

```python
import functools

import jax
import jax.numpy as jnp
from jax import lax
from jax.experimental import pallas as pl
from jax.experimental.pallas import tpu as pltpu
from jax.sharding import PartitionSpec as P

C_IN = 16
GROUPS = 32
COLS = 160
FR_DEV = 2
SEG = 16
LANES = 128
F32 = jnp.float32
BF16 = jnp.bfloat16


def band_kernel(w_ref, *refs):
    *vectors, o_ref, v_ref = refs
    for i, vector in enumerate(vectors):
        v_ref[i : i + 1, :] = vector[...].reshape(1, -1)
    o_ref[...] = jnp.zeros_like(o_ref)
    channels = w_ref.shape[1]
    depth = 3 * C_IN
    places = [(a, b, a, b) for a in range(3) for b in range(2)] + [(0, 2, 3, 0), (1, 2, 3, 1), (2, 2, 4, 0)]
    for a, b, group, side in places:
        for e in range(2):
            row = group * LANES + side * (LANES // 2) + e * C_IN
            tap = (a * 3 + b) * depth
            o_ref[row : row + depth, e * channels : (e + 1) * channels] = w_ref[tap : tap + depth, :]


def windows(e_ref, f_ref, pair, frames, high):
    (t0, t1), (h0, h1) = frames, high
    rows = slice(h0 * SEG, h1 * SEG)
    parts = [e_ref[pair, t0 + a : t1 + a, rows] for a in range(3)]
    parts.append(f_ref[pair, t0:t1, rows])
    parts.append(e_ref[pair, t0 + 2 : t1 + 2, (h0 + 2) * SEG : (h1 + 2) * SEG])
    size = (t1 - t0) * (h1 - h0) * SEG
    return jnp.concatenate([part.reshape(size, LANES) for part in parts], axis=1)


def fetch(sem, *pairs):
    copies = [pltpu.make_async_copy(source, target, sem.at[i]) for i, (source, target) in enumerate(pairs)]
    for copy in copies:
        copy.start()
    return copies


def lay_out(rows, own_ref, other_ref, halo_ref, z_ref, e_ref, f_ref):
    core = lax.rem(lax.axis_index("height"), 2)
    slots = 3 * rows
    per = COLS // SEG
    high = rows + 2

    for frame in range(6):
        for slot in (0, slots - 1):
            row = (frame * slots + slot) * SEG
            for half in range(2):
                z_ref[half, row : row + SEG, :] = jnp.zeros((SEG, LANES), F32)

    def spread(piece, frame, slot):
        base = pl.multiple_of((frame * slots + slot) * SEG, SEG)
        count = piece.shape[0]
        edge = jnp.zeros((count, LANES), F32)
        wide = jnp.concatenate([edge, piece, edge, edge], axis=1)
        for s in range(SEG):
            for half in range(2):
                start = LANES + s * per * C_IN - C_IN + half * 6 * C_IN
                lo = start // LANES * LANES
                window = wide[:, lo : lo + 2 * LANES]
                if start > lo:
                    window = pltpu.roll(window, 2 * LANES - (start - lo), 1)
                z_ref[half, pl.ds(base + s, count, stride=SEG), :] = window[:, :LANES]

    main = jnp.where(core == 0, rows, 0)
    edge_slot = jnp.where(core == 0, rows - 2, 2 * rows)
    for d in range(3):
        real = lax.axis_index("tm") >= 2 - d

        def piece(ref, *index):
            x = ref[(*index, d)].astype(F32)
            return x if d == 2 else jnp.where(real, x, 0.0)

        spread(piece(own_ref), 2 * d + core, main)
        spread(piece(other_ref), 2 * d + 1 - core, main)
        spread(piece(halo_ref, 0), 2 * d + 1 - core, edge_slot)
        spread(piece(halo_ref, 1), 2 * d + core, edge_slot)

    first = rows - 2
    span = rows + 4
    low_side = lax.broadcasted_iota(jnp.int32, (span * SEG, LANES), 1) < LANES // 2
    where = [(0, 0), (0, 2 * C_IN), (0, 4 * C_IN), (1, 0), (1, 2 * C_IN)]

    def turned(x, shift):
        return x if shift % LANES == 0 else pltpu.roll(x, shift % LANES, 1)

    for pair, (half, offset) in enumerate(where):
        upper = []
        for frame in range(6):
            x = z_ref[half, pl.ds((frame * slots + first) * SEG, (span + 1) * SEG), :]
            low, up = turned(x, -offset), turned(x, LANES // 2 - offset)
            e_ref[pair, frame] = jnp.where(low_side, low[: span * SEG], up[SEG:]).astype(BF16)
            if 0 < frame < 5:
                f_ref[pair, frame - 1] = jnp.where(
                    low_side[: high * SEG], upper, up[2 * SEG : span * SEG]
                ).astype(BF16)
            upper = low[2 * SEG : span * SEG]


def stats_kernel(rows, own_ref, other_ref, halo_ref, band_ref, v_ref, sum_ref, z_ref, e_ref, f_ref):
    lay_out(rows, own_ref, other_ref, halo_ref, z_ref, e_ref, f_ref)
    channels = v_ref.shape[1]
    per = COLS // SEG
    sums = jnp.zeros((8, 2 * channels), F32)
    squares = jnp.zeros((8, 2 * channels), F32)
    bias = jnp.concatenate([v_ref[0:1, :], v_ref[0:1, :]], axis=1)
    for pair in range(per // 2):
        out = jnp.dot(
            windows(e_ref, f_ref, pair, (2, 4), (1, 1 + rows)), band_ref[...], preferred_element_type=F32
        )
        out = (out + bias).reshape(-1, 8, 2 * channels)
        sums = sums + jnp.sum(out, axis=0)
        squares = squares + jnp.sum(out * out, axis=0)
    for i, part in enumerate((sums, squares)):
        whole = jnp.sum(part, axis=0, keepdims=True)
        whole = whole[:, :channels] + whole[:, channels:]
        sum_ref[:, 0, i * channels : (i + 1) * channels] = jnp.broadcast_to(whole, (sum_ref.shape[0], channels))


def opened_kernel(
    rows, own_ref, other_ref, halo_ref, band_ref, v_ref, first_ref, o_hbm, z_ref, e_ref, f_ref, o_ref, sem
):
    lay_out(rows, own_ref, other_ref, halo_ref, z_ref, e_ref, f_ref)
    channels = v_ref.shape[1]
    high = rows + 2
    stores = []
    for t0, t1 in ((2, 4), (1, 2), (0, 1)):
        here = pl.ds(t0 - 1, t1 - t0)
        for pair in range(COLS // SEG // 2):
            lhs = windows(e_ref, f_ref, pair, (t0, t1), (0, high))
            out = jnp.dot(lhs, band_ref[...], preferred_element_type=F32)
            for e in range(2):
                part = out[:, e * channels : (e + 1) * channels] + v_ref[0:1, :]
                part = part.reshape(t1 - t0, high, SEG, channels)
                if t0:
                    o_ref[here, :, 2 * pair + e] = part
                else:
                    first_ref[:, 2 * pair + e] = part[0]
        if t0:
            stores += fetch(sem.at[t0 - 1], (o_ref.at[here], o_hbm.at[here]))
    for store in stores:
        store.wait()


def second_kernel(
    rows, entries, sum_ref, first_ref, o_hbm, head_ref, w_hbm, v_ref, out_hbm,
    a_ref, place_ref, main_ref, two_ref, w_ref, o_ref, out_ref, sem,
):
    channels = v_ref.shape[1]
    per = COLS // SEG
    high = rows + 2
    third = 3 * channels
    weights = [
        pltpu.make_async_copy(w_hbm.at[pl.ds(i * third, third)], w_ref.at[pl.ds((i - 2) * third, third)], sem.at[i])
        for i in range(2, 9)
    ]
    loads = [pltpu.make_async_copy(o_hbm.at[t], o_ref.at[t], sem.at[9 + t]) for t in range(3)]
    for copy in (loads[0], *weights[:4], loads[1], *weights[4:], loads[2]):
        copy.start()
    height = lax.axis_index("height")
    frame = lax.axis_index("tm")
    group = channels // GROUPS
    left = jnp.floor((lax.broadcasted_iota(jnp.int32, (channels, channels), 0).astype(F32) + 0.5) / group)
    right = jnp.floor((lax.broadcasted_iota(jnp.int32, (channels, channels), 1).astype(F32) + 0.5) / group)
    same = jnp.where(left == right, 1.0, 0.0).astype(F32)
    total = jnp.sum(sum_ref[:, 0, :], axis=0, keepdims=True)
    both = jnp.concatenate([total[:, :channels], total[:, channels:], jnp.zeros((6, channels), F32)], axis=0)
    totals = jnp.dot(both, same, precision=lax.Precision.HIGHEST, preferred_element_type=F32)
    mean = totals[0:1] / entries
    var = totals[1:2] / entries - mean * mean
    scale = lax.rsqrt(var + 1e-06) * v_ref[1:2, :]
    half_scale = 0.5 * scale
    half_shift = 0.5 * (v_ref[2:3, :] - mean * scale)
    lane_row = lax.broadcasted_iota(jnp.int32, (SEG, channels), 0)

    def act_rows(t):
        return [functools.partial(act, t, h) for h in range(high)]

    def act(t, *hs):
        for h in hs or range(high):
            row = height * rows - 1 + h
            inside = (frame * FR_DEV - 2 + t >= 0) & (row >= 0) & (row < rows * lax.axis_size("height"))
            x = o_ref[t - 1, h] if t else first_ref[h]
            u = x.reshape(per * SEG, channels) * half_scale + half_shift
            y = u + u * jnp.tanh(u)
            y = jnp.where(inside, y, 0.0)
            a_ref[t, h, 1 : per + 1] = y.astype(BF16).reshape(per, SEG, channels)
            before = jnp.where(lane_row == 0, 0.0, pltpu.roll(y[(per - 1) * SEG :], 1, 0))
            after = jnp.where(lane_row == SEG - 1, 0.0, pltpu.roll(y[:SEG], SEG - 1, 0))
            a_ref[t, h, 0] = before.astype(BF16)
            a_ref[t, h, per + 1] = after.astype(BF16)

    wide = channels // (2 * LANES) * 2 * LANES

    def patch(frame, b, c, count):
        return a_ref[frame, b : b + rows, c : c + count].reshape(rows * count * SEG, channels)

    def tap(a, b, c, lanes):
        row = ((a * 3 + b) * 3 + c) * channels
        if row < head_ref.shape[0]:
            return head_ref[row : row + channels, lanes]
        row -= head_ref.shape[0]
        return w_ref[row : row + channels, lanes]

    def product(pairs, beside=()):
        beside = list(beside)
        acc = None
        for i in range(0, len(pairs), 2):
            some = pairs[i : i + 2]
            lhs = jnp.concatenate([x() for x, _ in some], axis=1)
            rhs = jnp.concatenate([y() for _, y in some], axis=0)
            part = jnp.dot(lhs, rhs, preferred_element_type=F32)
            acc = part if acc is None else acc + part
            if beside:
                beside.pop(0)()
        for step in beside:
            step()
        return acc

    low, rest = slice(0, wide), slice(wide, channels)

    def edge(t, a, start):
        f = t + a
        for i, (bs, beside) in enumerate(start):
            parts = (
                product([
                    (functools.partial(patch, f, b, c, per), functools.partial(tap, a, b, c, low))
                    for b in bs for c in range(3)
                ], beside),
                product([
                    (
                        functools.partial(patch, f, b, 0, per + 1),
                        lambda b=b: jnp.concatenate([tap(a, b, 0, rest), tap(a, b, 1, rest)], axis=1),
                    )
                    for b in bs
                ]),
                product([
                    (functools.partial(patch, f, b, 2, per), functools.partial(tap, a, b, 2, rest)) for b in bs
                ]),
            )
            if i == 0 and a == 0:
                main_ref[t, :, low], two_ref[t], main_ref[t, :, rest] = parts
            elif i == 0:
                two_ref[t] = parts[1]
                main_ref[t, :, low] += parts[0]
                main_ref[t, :, rest] += parts[2]
            else:
                two_ref[t] += parts[1]
                main_ref[t, :, low] += parts[0]
                main_ref[t, :, rest] += parts[2]

    def shared(f, beside):
        whole = slice(0, channels)
        both = product([
            (
                functools.partial(patch, f, b, c, per),
                lambda b=b, c=c: jnp.concatenate([tap(f, b, c, whole), tap(f - 1, b, c, whole)], axis=1),
            )
            for b in range(3) for c in range(3)
        ], beside)
        main_ref[0] += both[:, :channels]
        if f == 1:
            main_ref[1] = both[:, channels:]
        else:
            main_ref[1] += both[:, channels:]

    def finish(t):
        two = two_ref[t].reshape(rows, per + 1, SEG, 2 * LANES)
        size = rows * per * SEG
        main = main_ref[t, :, low]
        one = main_ref[t, :, rest]
        one = one + two[:, :per, :, :LANES].reshape(size, LANES) + two[:, 1:, :, LANES:].reshape(size, LANES)
        for h in range(rows):
            base = h * per * SEG
            opened = o_ref[t + 1, h + 1].reshape(per * SEG, channels)
            for tile in range(channels // LANES):
                lanes = slice(tile * LANES, (tile + 1) * LANES)
                source = main[:, lanes] if tile * LANES < wide else one
                whole = source[base : base + per * SEG] + v_ref[3:4, lanes] + opened[:, lanes]
                for k in range(per):
                    place_ref[t, h, tile, pl.ds(k, SEG, stride=per), :] = whole[k * SEG : (k + 1) * SEG]
                out_ref[t, h, :, lanes] = place_ref[t, h, tile].astype(BF16)
        store = pltpu.make_async_copy(out_ref.at[t], out_hbm.at[t], sem.at[14 + t])
        store.start()
        return store

    def need(*copies):
        for copy in copies:
            copy.wait()

    def steps(*parts):
        return [lambda group=group: [step() for step in group] for group in parts]

    rows1, rows2, rows3 = (act_rows(t) for t in (1, 2, 3))
    act(0)
    wait1 = functools.partial(need, weights[0], loads[0])
    wait2 = functools.partial(need, *weights[1:4], loads[1])
    wait3 = functools.partial(need, *weights[4:], loads[2])
    edge(0, 0, [((0, 1), steps([], [wait1])), ((2,), steps(rows1, [wait2]))])
    shared(1, steps(rows2, [wait3]))
    shared(2, steps(rows3))
    first = finish(0)
    edge(1, 2, [((0, 1, 2), [])])
    second = finish(1)
    need(first, second)


def second_part(rows, entries, sums, first, opened, head, weight, vectors):
    high, per, channels, frames = rows + 2, COLS // SEG, vectors.shape[1], FR_DEV
    vmem, hbm = pl.BlockSpec(memory_space=pltpu.VMEM), pl.BlockSpec(memory_space=pltpu.HBM)
    size = rows * per * SEG
    out_shape = (frames, rows, COLS, channels)
    return pl.pallas_call(
        functools.partial(second_kernel, rows, entries),
        out_shape=pltpu.HBM(out_shape, BF16),
        in_specs=[vmem, vmem, hbm, vmem, hbm, vmem],
        out_specs=hbm,
        scratch_shapes=[
            pltpu.VMEM((4, high, per + 2, SEG, channels), BF16),
            pltpu.VMEM((frames, rows, channels // LANES, COLS, LANES), F32),
            pltpu.VMEM((frames, size, channels), F32),
            pltpu.VMEM((frames, size // per * (per + 1), 2 * LANES), F32),
            pltpu.VMEM((weight.shape[0] - head.shape[0], channels), BF16),
            pltpu.VMEM(opened.shape, F32),
            pltpu.VMEM(out_shape, BF16),
            pltpu.SemaphoreType.DMA((16,)),
        ],
        compiler_params=pltpu.CompilerParams(vmem_limit_bytes=36 << 20),
        name="second",
    )(sums, first, opened, head, weight, vectors)


def shards(latent, in_weight, in_bias, norm_gain, norm_bias, conv_weight, conv_bias):
    frames = FR_DEV
    rows = latent.shape[0] // frames
    channels = conv_weight.shape[1]
    tm, height = lax.axis_size("tm"), lax.axis_size("height")
    half = height // 2
    core = lax.axis_index("height") % 2
    band, vectors = pl.pallas_call(
        band_kernel,
        out_shape=(
            pltpu.VMEM((5 * LANES, 2 * channels), BF16),
            pltpu.VMEM((4, channels), F32),
        ),
        name="band",
    )(in_weight, in_bias, norm_gain, norm_bias, conv_bias)

    received = []
    for d in (2, 1, 0):
        route = [
            (i * height + p * half + m, (i + d) % tm * height + 2 * m + p)
            for i in range(tm)
            for p in range(2)
            for m in range(half)
        ]
        received.append(lax.ppermute(latent, ("tm", "height"), route))
    own = jnp.stack(received)
    other = lax.ppermute(own, "height", [(i, i ^ 1) for i in range(height)])
    edge = lax.dynamic_slice_in_dim(jnp.stack([own, other]), core * (2 * rows - 2), 2, axis=2)
    swap = [(2 * m - 1, 2 * m) for m in range(1, half)] + [(2 * m, 2 * m - 1) for m in range(1, half)]
    halo = lax.ppermute(edge, "height", swap)

    per = COLS // SEG
    high = rows + 2
    vmem, hbm = pl.BlockSpec(memory_space=pltpu.VMEM), pl.BlockSpec(memory_space=pltpu.HBM)

    def keep(x):
        return pltpu.with_memory_space_constraint(x, pltpu.HBM)

    scratch = [
        pltpu.VMEM((2, 6 * 3 * rows * SEG, LANES), F32),
        pltpu.VMEM((per // 2, 6, (rows + 4) * SEG, LANES), BF16),
        pltpu.VMEM((per // 2, 4, high * SEG, LANES), BF16),
    ]
    sums = pl.pallas_call(
        functools.partial(stats_kernel, rows),
        out_shape=jax.ShapeDtypeStruct((tm * height, 1, 2 * channels), F32),
        in_specs=[vmem] * 5,
        scratch_shapes=scratch,
        compiler_params=pltpu.CompilerParams(vmem_limit_bytes=12 << 20),
        name="stats",
    )(own, other, halo, band, vectors)
    sums = lax.all_to_all(sums, ("tm", "height"), 0, 0, tiled=True)
    positions = 4 * high * per * SEG
    opened_shape = (3, high, per, SEG, channels)
    first, opened = pl.pallas_call(
        functools.partial(opened_kernel, rows),
        out_shape=(pltpu.VMEM(opened_shape[1:], F32), pltpu.HBM(opened_shape, F32)),
        in_specs=[vmem] * 5,
        out_specs=(vmem, hbm),
        scratch_shapes=[*scratch, pltpu.VMEM(opened_shape, F32), pltpu.SemaphoreType.DMA((2, 1))],
        cost_estimate=pl.CostEstimate(
            flops=2 * positions * 5 * LANES * channels, transcendentals=0, bytes_accessed=4 * positions * channels
        ),
        compiler_params=pltpu.CompilerParams(vmem_limit_bytes=16 << 20),
        name="opened",
    )(own, other, halo, band, vectors)
    entries = frames * tm * rows * height * COLS * (channels // GROUPS)
    head = pltpu.with_memory_space_constraint(conv_weight[: 6 * channels], pltpu.VMEM)
    return second_part(rows, entries, sums, first, keep(opened), head, keep(conv_weight), vectors)


def solution(mesh):
    return jax.shard_map(
        shards,
        mesh=mesh,
        in_specs=(P(("tm", "height"), None), P(), P(), P(), P(), P(), P()),
        out_specs=P("tm", "height", None, None),
        check_vma=False,
    )
```

```python
import functools

import jax
import jax.numpy as jnp
from jax import lax
from jax.experimental import pallas as pl
from jax.experimental.pallas import tpu as pltpu
from jax.sharding import PartitionSpec as P

C_IN = 16
GROUPS = 32
COLS = 160
FR_DEV = 2
SEG = 16
LANES = 128
F32 = jnp.float32
BF16 = jnp.bfloat16


def band_kernel(w_ref, *refs):
    *vectors, o_ref, v_ref = refs
    for i, vector in enumerate(vectors):
        v_ref[i : i + 1, :] = vector[...].reshape(1, -1)
    o_ref[...] = jnp.zeros_like(o_ref)
    channels = w_ref.shape[1]
    depth = 3 * C_IN
    places = [(a, b, a, b) for a in range(3) for b in range(2)] + [(0, 2, 3, 0), (1, 2, 3, 1), (2, 2, 4, 0)]
    for a, b, group, side in places:
        for e in range(2):
            row = group * LANES + side * (LANES // 2) + e * C_IN
            tap = (a * 3 + b) * depth
            o_ref[row : row + depth, e * channels : (e + 1) * channels] = w_ref[tap : tap + depth, :]


def windows(e_ref, f_ref, pair, frames, high):
    (t0, t1), (h0, h1) = frames, high
    rows = slice(h0 * SEG, h1 * SEG)
    parts = [e_ref[pair, t0 + a : t1 + a, rows] for a in range(3)]
    parts.append(f_ref[pair, t0:t1, rows])
    parts.append(e_ref[pair, t0 + 2 : t1 + 2, (h0 + 2) * SEG : (h1 + 2) * SEG])
    size = (t1 - t0) * (h1 - h0) * SEG
    return jnp.concatenate([part.reshape(size, LANES) for part in parts], axis=1)


def fetch(sem, *pairs):
    copies = [pltpu.make_async_copy(source, target, sem.at[i]) for i, (source, target) in enumerate(pairs)]
    for copy in copies:
        copy.start()
    return copies


def lay_out(rows, distances, own_ref, other_ref, halo_ref, z_ref, e_ref, f_ref):
    core = lax.rem(lax.axis_index("height"), 2)
    slots = 3 * rows
    per = COLS // SEG
    high = rows + 2

    frames = range(2 * distances[0], 6)
    for frame in frames:
        for slot in (0, slots - 1):
            row = (frame * slots + slot) * SEG
            for half in range(2):
                z_ref[half, row : row + SEG, :] = jnp.zeros((SEG, LANES), F32)

    def spread(piece, frame, slot):
        base = pl.multiple_of((frame * slots + slot) * SEG, SEG)
        count = piece.shape[0]
        edge = jnp.zeros((count, LANES), F32)
        wide = jnp.concatenate([edge, piece, edge, edge], axis=1)
        for s in range(SEG):
            for half in range(2):
                start = LANES + s * per * C_IN - C_IN + half * 6 * C_IN
                lo = start // LANES * LANES
                window = wide[:, lo : lo + 2 * LANES]
                if start > lo:
                    window = pltpu.roll(window, 2 * LANES - (start - lo), 1)
                z_ref[half, pl.ds(base + s, count, stride=SEG), :] = window[:, :LANES]

    main = jnp.where(core == 0, rows, 0)
    edge_slot = jnp.where(core == 0, rows - 2, 2 * rows)
    row_block, last_block = lax.axis_index("height"), lax.axis_size("height") - 1
    beside = jnp.where(core == 0, row_block > 0, row_block < last_block)
    for d in distances:
        real = lax.axis_index("tm") >= 2 - d

        def piece(ref, keep, *index):
            return jnp.where(keep, ref[(*index, d)].astype(F32), 0.0)

        spread(piece(own_ref, real), 2 * d + core, main)
        spread(piece(other_ref, real), 2 * d + 1 - core, main)
        spread(piece(halo_ref, real & beside, 0), 2 * d + core, edge_slot)
        spread(piece(halo_ref, real & beside, 1), 2 * d + 1 - core, edge_slot)

    first = rows - 2
    span = rows + 4
    low_side = lax.broadcasted_iota(jnp.int32, (span * SEG, LANES), 1) < LANES // 2
    where = [(0, 0), (0, 2 * C_IN), (0, 4 * C_IN), (1, 0), (1, 2 * C_IN)]

    def turned(x, shift):
        return x if shift % LANES == 0 else pltpu.roll(x, shift % LANES, 1)

    for pair, (half, offset) in enumerate(where):
        upper = []
        for frame in frames:
            x = z_ref[half, pl.ds((frame * slots + first) * SEG, (span + 1) * SEG), :]
            low, up = turned(x, -offset), turned(x, LANES // 2 - offset)
            e_ref[pair, frame] = jnp.where(low_side, low[: span * SEG], up[SEG:]).astype(BF16)
            if frames[0] < frame < 5:
                f_ref[pair, frame - 1] = jnp.where(
                    low_side[: high * SEG], upper, up[2 * SEG : span * SEG]
                ).astype(BF16)
            upper = low[2 * SEG : span * SEG]


def stats_kernel(rows, own_ref, other_ref, halo_ref, band_ref, v_ref, sum_ref, z_ref, e_ref, f_ref):
    lay_out(rows, (1, 2), own_ref, other_ref, halo_ref, z_ref, e_ref, f_ref)
    channels = v_ref.shape[1]
    per = COLS // SEG
    sums = jnp.zeros((8, 2 * channels), F32)
    squares = jnp.zeros((8, 2 * channels), F32)
    bias = jnp.concatenate([v_ref[0:1, :], v_ref[0:1, :]], axis=1)
    for pair in range(per // 2):
        out = jnp.dot(
            windows(e_ref, f_ref, pair, (2, 4), (1, 1 + rows)), band_ref[...], preferred_element_type=F32
        )
        out = (out + bias).reshape(-1, 8, 2 * channels)
        sums = sums + jnp.sum(out, axis=0)
        squares = squares + jnp.sum(out * out, axis=0)
    for i, part in enumerate((sums, squares)):
        whole = jnp.sum(part, axis=0, keepdims=True)
        whole = whole[:, :channels] + whole[:, channels:]
        sum_ref[:, 0, i * channels : (i + 1) * channels] = jnp.broadcast_to(whole, (sum_ref.shape[0], channels))


def opened_kernel(
    rows, own_ref, other_ref, halo_ref, band_ref, v_ref, first_ref, o_hbm, z_ref, e_ref, f_ref, o_ref, sem
):
    lay_out(rows, (0, 1, 2), own_ref, other_ref, halo_ref, z_ref, e_ref, f_ref)
    channels = v_ref.shape[1]
    high = rows + 2
    stores = []
    for t0, t1 in ((2, 4), (1, 2), (0, 1)):
        here = pl.ds(t0 - 1, t1 - t0)
        for pair in range(COLS // SEG // 2):
            lhs = windows(e_ref, f_ref, pair, (t0, t1), (0, high))
            out = jnp.dot(lhs, band_ref[...], preferred_element_type=F32)
            for e in range(2):
                part = out[:, e * channels : (e + 1) * channels] + v_ref[0:1, :]
                part = part.reshape(t1 - t0, high, SEG, channels)
                if t0:
                    o_ref[here, :, 2 * pair + e] = part
                else:
                    first_ref[:, 2 * pair + e] = part[0]
        if t0:
            stores += fetch(sem.at[t0 - 1], (o_ref.at[here], o_hbm.at[here]))
    for store in stores:
        store.wait()


def second_kernel(
    rows, entries, sum_ref, first_ref, o_hbm, head_ref, w_hbm, v_ref, out_hbm,
    a_ref, place_ref, main_ref, two_ref, w_ref, o_ref, out_ref, sem,
):
    channels = v_ref.shape[1]
    per = COLS // SEG
    high = rows + 2
    third = 3 * channels
    weights = [
        pltpu.make_async_copy(w_hbm.at[pl.ds(i * third, third)], w_ref.at[pl.ds((i - 2) * third, third)], sem.at[i])
        for i in range(2, 9)
    ]
    loads = [pltpu.make_async_copy(o_hbm.at[t], o_ref.at[t], sem.at[9 + t]) for t in range(3)]
    for copy in (loads[0], *weights[:4], loads[1], *weights[4:], loads[2]):
        copy.start()
    height = lax.axis_index("height")
    frame = lax.axis_index("tm")
    group = channels // GROUPS
    left = jnp.floor((lax.broadcasted_iota(jnp.int32, (channels, channels), 0).astype(F32) + 0.5) / group)
    right = jnp.floor((lax.broadcasted_iota(jnp.int32, (channels, channels), 1).astype(F32) + 0.5) / group)
    same = jnp.where(left == right, 1.0, 0.0).astype(F32)
    total = jnp.sum(sum_ref[:, 0, :], axis=0, keepdims=True)
    both = jnp.concatenate([total[:, :channels], total[:, channels:], jnp.zeros((6, channels), F32)], axis=0)
    totals = jnp.dot(both, same, precision=lax.Precision.HIGHEST, preferred_element_type=F32)
    mean = totals[0:1] / entries
    var = totals[1:2] / entries - mean * mean
    scale = lax.rsqrt(var + 1e-06) * v_ref[1:2, :]
    half_scale = 0.5 * scale
    half_shift = 0.5 * (v_ref[2:3, :] - mean * scale)
    lane_row = lax.broadcasted_iota(jnp.int32, (SEG, channels), 0)

    def act_rows(t):
        return [functools.partial(act, t, h) for h in range(high)]

    def act(t, *hs):
        for h in hs or range(high):
            row = height * rows - 1 + h
            inside = (frame * FR_DEV - 2 + t >= 0) & (row >= 0) & (row < rows * lax.axis_size("height"))
            x = o_ref[t - 1, h] if t else first_ref[h]
            u = x.reshape(per * SEG, channels) * half_scale + half_shift
            y = u + u * jnp.tanh(u)
            y = jnp.where(inside, y, 0.0)
            a_ref[t, h, 1 : per + 1] = y.astype(BF16).reshape(per, SEG, channels)
            before = jnp.where(lane_row == 0, 0.0, pltpu.roll(y[(per - 1) * SEG :], 1, 0))
            after = jnp.where(lane_row == SEG - 1, 0.0, pltpu.roll(y[:SEG], SEG - 1, 0))
            a_ref[t, h, 0] = before.astype(BF16)
            a_ref[t, h, per + 1] = after.astype(BF16)

    wide = channels // (2 * LANES) * 2 * LANES

    def patch(frame, b, c, count):
        return a_ref[frame, b : b + rows, c : c + count].reshape(rows * count * SEG, channels)

    def tap(a, b, c, lanes):
        row = ((a * 3 + b) * 3 + c) * channels
        if row < head_ref.shape[0]:
            return head_ref[row : row + channels, lanes]
        row -= head_ref.shape[0]
        return w_ref[row : row + channels, lanes]

    def product(pairs, beside=()):
        beside = list(beside)
        acc = None
        for i in range(0, len(pairs), 2):
            some = pairs[i : i + 2]
            lhs = jnp.concatenate([x() for x, _ in some], axis=1)
            rhs = jnp.concatenate([y() for _, y in some], axis=0)
            part = jnp.dot(lhs, rhs, preferred_element_type=F32)
            acc = part if acc is None else acc + part
            if beside:
                beside.pop(0)()
        for step in beside:
            step()
        return acc

    low, rest = slice(0, wide), slice(wide, channels)

    def edge(t, a, start):
        f = t + a
        for i, (bs, beside) in enumerate(start):
            parts = (
                product([
                    (functools.partial(patch, f, b, c, per), functools.partial(tap, a, b, c, low))
                    for b in bs for c in range(3)
                ], beside),
                product([
                    (
                        functools.partial(patch, f, b, 0, per + 1),
                        lambda b=b: jnp.concatenate([tap(a, b, 0, rest), tap(a, b, 1, rest)], axis=1),
                    )
                    for b in bs
                ]),
                product([
                    (functools.partial(patch, f, b, 2, per), functools.partial(tap, a, b, 2, rest)) for b in bs
                ]),
            )
            if i == 0 and a == 0:
                main_ref[t, :, low], two_ref[t], main_ref[t, :, rest] = parts
            elif i == 0:
                two_ref[t] = parts[1]
                main_ref[t, :, low] += parts[0]
                main_ref[t, :, rest] += parts[2]
            else:
                two_ref[t] += parts[1]
                main_ref[t, :, low] += parts[0]
                main_ref[t, :, rest] += parts[2]

    def shared(f, beside):
        whole = slice(0, channels)
        both = product([
            (
                functools.partial(patch, f, b, c, per),
                lambda b=b, c=c: jnp.concatenate([tap(f, b, c, whole), tap(f - 1, b, c, whole)], axis=1),
            )
            for b in range(3) for c in range(3)
        ], beside)
        main_ref[0] += both[:, :channels]
        if f == 1:
            main_ref[1] = both[:, channels:]
        else:
            main_ref[1] += both[:, channels:]

    def finish(t):
        two = two_ref[t].reshape(rows, per + 1, SEG, 2 * LANES)
        size = rows * per * SEG
        main = main_ref[t, :, low]
        one = main_ref[t, :, rest]
        one = one + two[:, :per, :, :LANES].reshape(size, LANES) + two[:, 1:, :, LANES:].reshape(size, LANES)
        for h in range(rows):
            base = h * per * SEG
            opened = o_ref[t + 1, h + 1].reshape(per * SEG, channels)
            for tile in range(channels // LANES):
                lanes = slice(tile * LANES, (tile + 1) * LANES)
                source = main[:, lanes] if tile * LANES < wide else one
                whole = source[base : base + per * SEG] + v_ref[3:4, lanes] + opened[:, lanes]
                for k in range(per):
                    place_ref[t, h, tile, pl.ds(k, SEG, stride=per), :] = whole[k * SEG : (k + 1) * SEG]
                out_ref[t, h, :, lanes] = place_ref[t, h, tile].astype(BF16)
        store = pltpu.make_async_copy(out_ref.at[t], out_hbm.at[t], sem.at[14 + t])
        store.start()
        return store

    def need(*copies):
        for copy in copies:
            copy.wait()

    def steps(*parts):
        return [lambda group=group: [step() for step in group] for group in parts]

    rows1, rows2, rows3 = (act_rows(t) for t in (1, 2, 3))
    act(0)
    wait1 = functools.partial(need, weights[0], loads[0])
    wait2 = functools.partial(need, *weights[1:4], loads[1])
    wait3 = functools.partial(need, *weights[4:], loads[2])
    wait3a = functools.partial(need, *weights[4:])
    wait3b = functools.partial(need, loads[2])
    edge(0, 0, [((0, 1), steps([], [], [wait1])), ((2,), steps(rows1, [wait2]))])
    shared(1, steps(rows2, [wait3]))
    shared(2, steps(rows3))
    first = finish(0)
    edge(1, 2, [((0, 1, 2), [])])
    second = finish(1)
    need(first, second)


def second_part(rows, entries, sums, first, opened, head, weight, vectors):
    high, per, channels, frames = rows + 2, COLS // SEG, vectors.shape[1], FR_DEV
    vmem, hbm = pl.BlockSpec(memory_space=pltpu.VMEM), pl.BlockSpec(memory_space=pltpu.HBM)
    size = rows * per * SEG
    out_shape = (frames, rows, COLS, channels)
    return pl.pallas_call(
        functools.partial(second_kernel, rows, entries),
        out_shape=pltpu.HBM(out_shape, BF16),
        in_specs=[vmem, vmem, hbm, vmem, hbm, vmem],
        out_specs=hbm,
        scratch_shapes=[
            pltpu.VMEM((4, high, per + 2, SEG, channels), BF16),
            pltpu.VMEM((frames, rows, channels // LANES, COLS, LANES), F32),
            pltpu.VMEM((frames, size, channels), F32),
            pltpu.VMEM((frames, size // per * (per + 1), 2 * LANES), F32),
            pltpu.VMEM((weight.shape[0] - head.shape[0], channels), BF16),
            pltpu.VMEM(opened.shape, F32),
            pltpu.VMEM(out_shape, BF16),
            pltpu.SemaphoreType.DMA((16,)),
        ],
        compiler_params=pltpu.CompilerParams(vmem_limit_bytes=36 << 20),
        name="second",
    )(sums, first, opened, head, weight, vectors)


def shards(latent, in_weight, in_bias, norm_gain, norm_bias, conv_weight, conv_bias):
    frames = FR_DEV
    rows = latent.shape[0] // frames
    channels = conv_weight.shape[1]
    tm, height = lax.axis_size("tm"), lax.axis_size("height")
    half = height // 2
    core = lax.axis_index("height") % 2
    band, vectors = pl.pallas_call(
        band_kernel,
        out_shape=(
            pltpu.VMEM((5 * LANES, 2 * channels), BF16),
            pltpu.VMEM((4, channels), F32),
        ),
        name="band",
    )(in_weight, in_bias, norm_gain, norm_bias, conv_bias)

    received = []
    for d in (2, 1, 0):
        route = [
            (i * height + p * half + m, (i + d) % tm * height + 2 * m + p)
            for i in range(tm)
            for p in range(2)
            for m in range(half)
        ]
        received.append(lax.ppermute(latent, ("tm", "height"), route))
    own = jnp.stack(received)
    other = lax.ppermute(own, "height", [(i, i ^ 1) for i in range(height)])
    edge = lax.dynamic_slice_in_dim(jnp.stack([own, other]), (1 - core) * (2 * rows - 2), 2, axis=2)
    down = [(2 * m, 2 * m + 2) for m in range(half - 1)] + [(height - 2, height - 1)]
    up = [(2 * m + 1, 2 * m - 1) for m in range(1, half)] + [(1, 0)]
    halo = lax.ppermute(edge, "height", down + up)

    per = COLS // SEG
    high = rows + 2
    vmem, hbm = pl.BlockSpec(memory_space=pltpu.VMEM), pl.BlockSpec(memory_space=pltpu.HBM)

    def keep(x):
        return pltpu.with_memory_space_constraint(x, pltpu.HBM)

    scratch = [
        pltpu.VMEM((2, 6 * 3 * rows * SEG, LANES), F32),
        pltpu.VMEM((per // 2, 6, (rows + 4) * SEG, LANES), BF16),
        pltpu.VMEM((per // 2, 4, high * SEG, LANES), BF16),
    ]
    sums = pl.pallas_call(
        functools.partial(stats_kernel, rows),
        out_shape=jax.ShapeDtypeStruct((tm * height, 1, 2 * channels), F32),
        in_specs=[vmem] * 5,
        scratch_shapes=scratch,
        compiler_params=pltpu.CompilerParams(vmem_limit_bytes=12 << 20),
        name="stats",
    )(own, other, halo, band, vectors)
    sums = lax.all_to_all(sums, ("tm", "height"), 0, 0, tiled=True)
    positions = 4 * high * per * SEG
    opened_shape = (3, high, per, SEG, channels)
    first, opened = pl.pallas_call(
        functools.partial(opened_kernel, rows),
        out_shape=(pltpu.VMEM(opened_shape[1:], F32), pltpu.HBM(opened_shape, F32)),
        in_specs=[vmem] * 5,
        out_specs=(vmem, hbm),
        scratch_shapes=[*scratch, pltpu.VMEM(opened_shape, F32), pltpu.SemaphoreType.DMA((2, 1))],
        cost_estimate=pl.CostEstimate(
            flops=2 * positions * 5 * LANES * channels, transcendentals=0, bytes_accessed=4 * positions * channels
        ),
        compiler_params=pltpu.CompilerParams(vmem_limit_bytes=16 << 20),
        name="opened",
    )(own, other, halo, band, vectors)
    entries = frames * tm * rows * height * COLS * (channels // GROUPS)
    head = pltpu.with_memory_space_constraint(conv_weight[: 6 * channels], pltpu.VMEM)
    return second_part(rows, entries, sums, first, keep(opened), head, keep(conv_weight), vectors)


def solution(mesh):
    return jax.shard_map(
        shards,
        mesh=mesh,
        in_specs=(P(("tm", "height"), None), P(), P(), P(), P(), P(), P()),
        out_specs=P("tm", "height", None, None),
        check_vma=False,
    )
```

```python
import functools

import jax
import jax.numpy as jnp
from jax import lax
from jax.experimental import pallas as pl
from jax.experimental.pallas import tpu as pltpu
from jax.sharding import PartitionSpec as P

C_IN = 16
GROUPS = 32
COLS = 160
FR_DEV = 2
SEG = 16
LANES = 128
F32 = jnp.float32
BF16 = jnp.bfloat16


def band_kernel(w_ref, *refs):
    *vectors, o_ref, v_ref = refs
    for i, vector in enumerate(vectors):
        v_ref[i : i + 1, :] = vector[...].reshape(1, -1)
    o_ref[...] = jnp.zeros_like(o_ref)
    channels = w_ref.shape[1]
    depth = 3 * C_IN
    places = [(a, b, a, b) for a in range(3) for b in range(2)] + [(0, 2, 3, 0), (1, 2, 3, 1), (2, 2, 4, 0)]
    for a, b, group, side in places:
        for e in range(2):
            row = group * LANES + side * (LANES // 2) + e * C_IN
            tap = (a * 3 + b) * depth
            o_ref[row : row + depth, e * channels : (e + 1) * channels] = w_ref[tap : tap + depth, :]


def windows(e_ref, f_ref, pair, frames, high):
    (t0, t1), (h0, h1) = frames, high
    rows = slice(h0 * SEG, h1 * SEG)
    parts = [e_ref[pair, t0 + a : t1 + a, rows] for a in range(3)]
    parts.append(f_ref[pair, t0:t1, rows])
    parts.append(e_ref[pair, t0 + 2 : t1 + 2, (h0 + 2) * SEG : (h1 + 2) * SEG])
    size = (t1 - t0) * (h1 - h0) * SEG
    return jnp.concatenate([part.reshape(size, LANES) for part in parts], axis=1)


def fetch(sem, *pairs):
    copies = [pltpu.make_async_copy(source, target, sem.at[i]) for i, (source, target) in enumerate(pairs)]
    for copy in copies:
        copy.start()
    return copies


def lay_out(rows, distances, own_ref, other_ref, halo_ref, z_ref, e_ref, f_ref):
    core = lax.rem(lax.axis_index("height"), 2)
    slots = 3 * rows
    per = COLS // SEG
    high = rows + 2

    frames = range(2 * distances[0], 6)
    for frame in frames:
        for slot in (0, slots - 1):
            row = (frame * slots + slot) * SEG
            for half in range(2):
                z_ref[half, row : row + SEG, :] = jnp.zeros((SEG, LANES), F32)

    def spread(piece, frame, slot):
        base = pl.multiple_of((frame * slots + slot) * SEG, SEG)
        count = piece.shape[0]
        edge = jnp.zeros((count, LANES), F32)
        wide = jnp.concatenate([edge, piece, edge, edge], axis=1)
        for s in range(SEG):
            for half in range(2):
                start = LANES + s * per * C_IN - C_IN + half * 6 * C_IN
                lo = start // LANES * LANES
                window = wide[:, lo : lo + 2 * LANES]
                if start > lo:
                    window = pltpu.roll(window, 2 * LANES - (start - lo), 1)
                z_ref[half, pl.ds(base + s, count, stride=SEG), :] = window[:, :LANES]

    main = jnp.where(core == 0, rows, 0)
    edge_slot = jnp.where(core == 0, rows - 2, 2 * rows)
    row_block, last_block = lax.axis_index("height"), lax.axis_size("height") - 1
    beside = jnp.where(core == 0, row_block > 0, row_block < last_block)
    for d in distances:
        real = lax.axis_index("tm") >= 2 - d

        def piece(ref, keep, *index):
            return jnp.where(keep, ref[(*index, d)].astype(F32), 0.0)

        spread(piece(own_ref, real), 2 * d + core, main)
        spread(piece(other_ref, real), 2 * d + 1 - core, main)
        spread(piece(halo_ref, real & beside, 0), 2 * d + core, edge_slot)
        spread(piece(halo_ref, real & beside, 1), 2 * d + 1 - core, edge_slot)

    first = rows - 2
    span = rows + 4
    low_side = lax.broadcasted_iota(jnp.int32, (span * SEG, LANES), 1) < LANES // 2
    where = [(0, 0), (0, 2 * C_IN), (0, 4 * C_IN), (1, 0), (1, 2 * C_IN)]

    def turned(x, shift):
        return x if shift % LANES == 0 else pltpu.roll(x, shift % LANES, 1)

    for pair, (half, offset) in enumerate(where):
        upper = []
        for frame in frames:
            x = z_ref[half, pl.ds((frame * slots + first) * SEG, (span + 1) * SEG), :]
            low, up = turned(x, -offset), turned(x, LANES // 2 - offset)
            e_ref[pair, frame] = jnp.where(low_side, low[: span * SEG], up[SEG:]).astype(BF16)
            if frames[0] < frame < 5:
                f_ref[pair, frame - 1] = jnp.where(
                    low_side[: high * SEG], upper, up[2 * SEG : span * SEG]
                ).astype(BF16)
            upper = low[2 * SEG : span * SEG]


def exact_product(rows, member):
    parts = []
    for x in rows:
        for _ in range(3):
            part = x.astype(BF16).astype(F32)
            parts.append(part)
            x = x - part
    parts.append(jnp.zeros((16 - len(parts), x.shape[1]), F32))
    out = jnp.dot(jnp.concatenate(parts, axis=0).astype(BF16), member.astype(BF16), preferred_element_type=F32)
    return [out[3 * i : 3 * i + 1] + out[3 * i + 1 : 3 * i + 2] + out[3 * i + 2 : 3 * i + 3] for i in range(len(rows))]


def stats_kernel(rows, own_ref, other_ref, halo_ref, band_ref, v_ref, sum_ref, z_ref, e_ref, f_ref):
    lay_out(rows, (1, 2), own_ref, other_ref, halo_ref, z_ref, e_ref, f_ref)
    channels = v_ref.shape[1]
    per = COLS // SEG
    sums = jnp.zeros((8, 2 * channels), F32)
    squares = jnp.zeros((8, 2 * channels), F32)
    bias = jnp.concatenate([v_ref[0:1, :], v_ref[0:1, :]], axis=1)
    for pair in range(per // 2):
        out = jnp.dot(
            windows(e_ref, f_ref, pair, (2, 4), (1, 1 + rows)), band_ref[...], preferred_element_type=F32
        )
        out = (out + bias).reshape(-1, 8, 2 * channels)
        sums = sums + jnp.sum(out, axis=0)
        squares = squares + jnp.sum(out * out, axis=0)
    whole = []
    for part in (sums, squares):
        row = jnp.sum(part, axis=0, keepdims=True)
        whole.append(row[:, :channels] + row[:, channels:])
    size = channels // GROUPS
    row = lax.broadcasted_iota(jnp.int32, (channels, LANES), 0)
    first = lax.rem(lax.broadcasted_iota(jnp.int32, (channels, LANES), 1), GROUPS) * size
    member = jnp.where((row >= first) & (row < first + size), 1.0, 0.0)
    per_group = exact_product(whole, member)
    lane = lax.broadcasted_iota(jnp.int32, (1, LANES), 1)
    payload = jnp.where(lane < GROUPS, per_group[0], per_group[1])
    sum_ref[:, 0, :] = jnp.broadcast_to(payload, (sum_ref.shape[0], LANES))


def opened_kernel(
    rows, own_ref, other_ref, halo_ref, band_ref, v_ref, first_ref, o_hbm, z_ref, e_ref, f_ref, o_ref, sem
):
    lay_out(rows, (0, 1, 2), own_ref, other_ref, halo_ref, z_ref, e_ref, f_ref)
    channels = v_ref.shape[1]
    high = rows + 2
    stores = []
    for t0, t1 in ((2, 4), (1, 2), (0, 1)):
        here = pl.ds(t0 - 1, t1 - t0)
        for pair in range(COLS // SEG // 2):
            lhs = windows(e_ref, f_ref, pair, (t0, t1), (0, high))
            out = jnp.dot(lhs, band_ref[...], preferred_element_type=F32)
            for e in range(2):
                part = out[:, e * channels : (e + 1) * channels] + v_ref[0:1, :]
                part = part.reshape(t1 - t0, high, SEG, channels)
                if t0:
                    o_ref[here, :, 2 * pair + e] = part
                else:
                    first_ref[:, 2 * pair + e] = part[0]
        if t0:
            stores += fetch(sem.at[t0 - 1], (o_ref.at[here], o_hbm.at[here]))
    for store in stores:
        store.wait()


def second_kernel(
    rows, entries, sum_ref, first_ref, o_hbm, head_ref, w_hbm, v_ref, out_hbm,
    a_ref, place_ref, main_ref, two_ref, w_ref, o_ref, out_ref, sem,
):
    channels = v_ref.shape[1]
    per = COLS // SEG
    high = rows + 2
    third = 3 * channels
    weights = [
        pltpu.make_async_copy(w_hbm.at[pl.ds(i * third, third)], w_ref.at[pl.ds((i - 2) * third, third)], sem.at[i])
        for i in range(2, 9)
    ]
    loads = [pltpu.make_async_copy(o_hbm.at[t], o_ref.at[t], sem.at[9 + t]) for t in range(3)]
    for copy in (loads[0], *weights[:4], loads[1], *weights[4:], loads[2]):
        copy.start()
    height = lax.axis_index("height")
    frame = lax.axis_index("tm")
    size = channels // GROUPS
    lane = lax.broadcasted_iota(jnp.int32, (1, LANES), 1)
    total = jnp.sum(sum_ref[:, 0, :], axis=0, keepdims=True)
    mean = total / entries
    var = pltpu.roll(mean, LANES - GROUPS, 1) - mean * mean
    inverse = lax.rsqrt(jnp.where(lane < GROUPS, var, 1.0) + 1e-06)
    first = lax.broadcasted_iota(jnp.int32, (LANES, channels), 0) * size
    column = lax.broadcasted_iota(jnp.int32, (LANES, channels), 1)
    member = jnp.where((column >= first) & (column < first + size), 1.0, 0.0)
    mean, inverse = exact_product([mean, inverse], member)
    scale = inverse * v_ref[1:2, :]
    half_scale = 0.5 * scale
    half_shift = 0.5 * (v_ref[2:3, :] - mean * scale)
    lane_row = lax.broadcasted_iota(jnp.int32, (SEG, channels), 0)

    def act_rows(t):
        return [functools.partial(act, t, h) for h in range(high)]

    def act(t, *hs):
        for h in hs or range(high):
            row = height * rows - 1 + h
            inside = (frame * FR_DEV - 2 + t >= 0) & (row >= 0) & (row < rows * lax.axis_size("height"))
            x = o_ref[t - 1, h] if t else first_ref[h]
            u = x.reshape(per * SEG, channels) * half_scale + half_shift
            y = u + u * jnp.tanh(u)
            y = jnp.where(inside, y, 0.0)
            a_ref[t, h, 1 : per + 1] = y.astype(BF16).reshape(per, SEG, channels)
            before = jnp.where(lane_row == 0, 0.0, pltpu.roll(y[(per - 1) * SEG :], 1, 0))
            after = jnp.where(lane_row == SEG - 1, 0.0, pltpu.roll(y[:SEG], SEG - 1, 0))
            a_ref[t, h, 0] = before.astype(BF16)
            a_ref[t, h, per + 1] = after.astype(BF16)

    wide = channels // (2 * LANES) * 2 * LANES

    def patch(frame, b, c, count):
        return a_ref[frame, b : b + rows, c : c + count].reshape(rows * count * SEG, channels)

    def tap(a, b, c, lanes):
        row = ((a * 3 + b) * 3 + c) * channels
        if row < head_ref.shape[0]:
            return head_ref[row : row + channels, lanes]
        row -= head_ref.shape[0]
        return w_ref[row : row + channels, lanes]

    def product(pairs, beside=()):
        beside = list(beside)
        acc = None
        for i in range(0, len(pairs), 2):
            some = pairs[i : i + 2]
            lhs = jnp.concatenate([x() for x, _ in some], axis=1)
            rhs = jnp.concatenate([y() for _, y in some], axis=0)
            part = jnp.dot(lhs, rhs, preferred_element_type=F32)
            acc = part if acc is None else acc + part
            if beside:
                beside.pop(0)()
        for step in beside:
            step()
        return acc

    low, rest = slice(0, wide), slice(wide, channels)

    def edge(t, a, start):
        f = t + a
        for i, (bs, beside) in enumerate(start):
            parts = (
                product([
                    (functools.partial(patch, f, b, c, per), functools.partial(tap, a, b, c, low))
                    for b in bs for c in range(3)
                ], beside),
                product([
                    (
                        functools.partial(patch, f, b, 0, per + 1),
                        lambda b=b: jnp.concatenate([tap(a, b, 0, rest), tap(a, b, 1, rest)], axis=1),
                    )
                    for b in bs
                ]),
                product([
                    (functools.partial(patch, f, b, 2, per), functools.partial(tap, a, b, 2, rest)) for b in bs
                ]),
            )
            if i == 0 and a == 0:
                main_ref[t, :, low], two_ref[t], main_ref[t, :, rest] = parts
            elif i == 0:
                two_ref[t] = parts[1]
                main_ref[t, :, low] += parts[0]
                main_ref[t, :, rest] += parts[2]
            else:
                two_ref[t] += parts[1]
                main_ref[t, :, low] += parts[0]
                main_ref[t, :, rest] += parts[2]

    def shared(f, beside):
        whole = slice(0, channels)
        both = product([
            (
                functools.partial(patch, f, b, c, per),
                lambda b=b, c=c: jnp.concatenate([tap(f, b, c, whole), tap(f - 1, b, c, whole)], axis=1),
            )
            for b in range(3) for c in range(3)
        ], beside)
        main_ref[0] += both[:, :channels]
        if f == 1:
            main_ref[1] = both[:, channels:]
        else:
            main_ref[1] += both[:, channels:]

    def finish(t):
        two = two_ref[t].reshape(rows, per + 1, SEG, 2 * LANES)
        size = rows * per * SEG
        main = main_ref[t, :, low]
        one = main_ref[t, :, rest]
        one = one + two[:, :per, :, :LANES].reshape(size, LANES) + two[:, 1:, :, LANES:].reshape(size, LANES)
        for h in range(rows):
            base = h * per * SEG
            opened = o_ref[t + 1, h + 1].reshape(per * SEG, channels)
            for tile in range(channels // LANES):
                lanes = slice(tile * LANES, (tile + 1) * LANES)
                source = main[:, lanes] if tile * LANES < wide else one
                whole = source[base : base + per * SEG] + v_ref[3:4, lanes] + opened[:, lanes]
                for k in range(per):
                    place_ref[t, h, tile, pl.ds(k, SEG, stride=per), :] = whole[k * SEG : (k + 1) * SEG]
                out_ref[t, h, :, lanes] = place_ref[t, h, tile].astype(BF16)
        store = pltpu.make_async_copy(out_ref.at[t], out_hbm.at[t], sem.at[14 + t])
        store.start()
        return store

    def need(*copies):
        for copy in copies:
            copy.wait()

    def steps(*parts):
        return [lambda group=group: [step() for step in group] for group in parts]

    rows1, rows2, rows3 = (act_rows(t) for t in (1, 2, 3))
    act(0)
    wait1 = functools.partial(need, weights[0], loads[0])
    wait2 = functools.partial(need, *weights[1:4], loads[1])
    wait3 = functools.partial(need, *weights[4:], loads[2])
    wait3a = functools.partial(need, *weights[4:])
    wait3b = functools.partial(need, loads[2])
    edge(0, 0, [((0, 1), steps([], [], [wait1])), ((2,), steps(rows1, [wait2]))])
    shared(1, steps(rows2, [wait3]))
    shared(2, steps(rows3))
    first = finish(0)
    edge(1, 2, [((0, 1, 2), [])])
    second = finish(1)
    need(first, second)


def second_part(rows, entries, sums, first, opened, head, weight, vectors):
    high, per, channels, frames = rows + 2, COLS // SEG, vectors.shape[1], FR_DEV
    vmem, hbm = pl.BlockSpec(memory_space=pltpu.VMEM), pl.BlockSpec(memory_space=pltpu.HBM)
    size = rows * per * SEG
    out_shape = (frames, rows, COLS, channels)
    return pl.pallas_call(
        functools.partial(second_kernel, rows, entries),
        out_shape=pltpu.HBM(out_shape, BF16),
        in_specs=[vmem, vmem, hbm, vmem, hbm, vmem],
        out_specs=hbm,
        scratch_shapes=[
            pltpu.VMEM((4, high, per + 2, SEG, channels), BF16),
            pltpu.VMEM((frames, rows, channels // LANES, COLS, LANES), F32),
            pltpu.VMEM((frames, size, channels), F32),
            pltpu.VMEM((frames, size // per * (per + 1), 2 * LANES), F32),
            pltpu.VMEM((weight.shape[0] - head.shape[0], channels), BF16),
            pltpu.VMEM(opened.shape, F32),
            pltpu.VMEM(out_shape, BF16),
            pltpu.SemaphoreType.DMA((16,)),
        ],
        compiler_params=pltpu.CompilerParams(vmem_limit_bytes=36 << 20),
        name="second",
    )(sums, first, opened, head, weight, vectors)


def shards(latent, in_weight, in_bias, norm_gain, norm_bias, conv_weight, conv_bias):
    frames = FR_DEV
    rows = latent.shape[0] // frames
    channels = conv_weight.shape[1]
    tm, height = lax.axis_size("tm"), lax.axis_size("height")
    half = height // 2
    core = lax.axis_index("height") % 2
    band, vectors = pl.pallas_call(
        band_kernel,
        out_shape=(
            pltpu.VMEM((5 * LANES, 2 * channels), BF16),
            pltpu.VMEM((4, channels), F32),
        ),
        name="band",
    )(in_weight, in_bias, norm_gain, norm_bias, conv_bias)

    received = []
    for d in (2, 1, 0):
        route = [
            (i * height + p * half + m, (i + d) % tm * height + 2 * m + p)
            for i in range(tm)
            for p in range(2)
            for m in range(half)
        ]
        received.append(lax.ppermute(latent, ("tm", "height"), route))
    own = jnp.stack(received)
    other = lax.ppermute(own, "height", [(i, i ^ 1) for i in range(height)])
    edge = lax.dynamic_slice_in_dim(jnp.stack([own, other]), (1 - core) * (2 * rows - 2), 2, axis=2)
    down = [(2 * m, 2 * m + 2) for m in range(half - 1)] + [(height - 2, height - 1)]
    up = [(2 * m + 1, 2 * m - 1) for m in range(1, half)] + [(1, 0)]
    halo = lax.ppermute(edge, "height", down + up)

    per = COLS // SEG
    high = rows + 2
    vmem, hbm = pl.BlockSpec(memory_space=pltpu.VMEM), pl.BlockSpec(memory_space=pltpu.HBM)

    def keep(x):
        return pltpu.with_memory_space_constraint(x, pltpu.HBM)

    scratch = [
        pltpu.VMEM((2, 6 * 3 * rows * SEG, LANES), F32),
        pltpu.VMEM((per // 2, 6, (rows + 4) * SEG, LANES), BF16),
        pltpu.VMEM((per // 2, 4, high * SEG, LANES), BF16),
    ]
    sums = pl.pallas_call(
        functools.partial(stats_kernel, rows),
        out_shape=jax.ShapeDtypeStruct((tm * height, 1, LANES), F32),
        in_specs=[vmem] * 5,
        scratch_shapes=scratch,
        compiler_params=pltpu.CompilerParams(vmem_limit_bytes=12 << 20),
        name="stats",
    )(own, other, halo, band, vectors)
    sums, later_weight = lax.optimization_barrier((sums, conv_weight))
    sums = lax.all_to_all(sums, ("tm", "height"), 0, 0, tiled=True)
    positions = 4 * high * per * SEG
    opened_shape = (3, high, per, SEG, channels)
    first, opened = pl.pallas_call(
        functools.partial(opened_kernel, rows),
        out_shape=(pltpu.VMEM(opened_shape[1:], F32), pltpu.HBM(opened_shape, F32)),
        in_specs=[vmem] * 5,
        out_specs=(vmem, hbm),
        scratch_shapes=[*scratch, pltpu.VMEM(opened_shape, F32), pltpu.SemaphoreType.DMA((2, 1))],
        cost_estimate=pl.CostEstimate(
            flops=2 * positions * 5 * LANES * channels, transcendentals=0, bytes_accessed=4 * positions * channels
        ),
        compiler_params=pltpu.CompilerParams(vmem_limit_bytes=16 << 20),
        name="opened",
    )(own, other, halo, band, vectors)
    entries = frames * tm * rows * height * COLS * (channels // GROUPS)
    head = pltpu.with_memory_space_constraint(later_weight[: 6 * channels], pltpu.VMEM)
    return second_part(rows, entries, sums, first, keep(opened), head, keep(conv_weight), vectors)


def solution(mesh):
    return jax.shard_map(
        shards,
        mesh=mesh,
        in_specs=(P(("tm", "height"), None), P(), P(), P(), P(), P(), P()),
        out_specs=P("tm", "height", None, None),
        check_vma=False,
    )
```

```python
import functools

import jax
import jax.numpy as jnp
from jax import lax
from jax.experimental import pallas as pl
from jax.experimental.pallas import tpu as pltpu
from jax.sharding import PartitionSpec as P

C_IN = 16
GROUPS = 32
COLS = 160
FR_DEV = 2
SEG = 16
LANES = 128
F32 = jnp.float32
BF16 = jnp.bfloat16


def band_kernel(w_ref, *refs):
    *vectors, o_ref, v_ref = refs
    for i, vector in enumerate(vectors):
        v_ref[i : i + 1, :] = vector[...].reshape(1, -1)
    o_ref[...] = jnp.zeros_like(o_ref)
    channels = w_ref.shape[1]
    depth = 3 * C_IN
    places = [(a, b, a, b) for a in range(3) for b in range(2)] + [(0, 2, 3, 0), (1, 2, 3, 1), (2, 2, 4, 0)]
    for a, b, group, side in places:
        for e in range(2):
            row = group * LANES + side * (LANES // 2) + e * C_IN
            tap = (a * 3 + b) * depth
            o_ref[row : row + depth, e * channels : (e + 1) * channels] = w_ref[tap : tap + depth, :]


def windows(e_ref, f_ref, pair, frames, high):
    (t0, t1), (h0, h1) = frames, high
    rows = slice(h0 * SEG, h1 * SEG)
    parts = [e_ref[pair, t0 + a : t1 + a, rows] for a in range(3)]
    parts.append(f_ref[pair, t0:t1, rows])
    parts.append(e_ref[pair, t0 + 2 : t1 + 2, (h0 + 2) * SEG : (h1 + 2) * SEG])
    size = (t1 - t0) * (h1 - h0) * SEG
    return jnp.concatenate([part.reshape(size, LANES) for part in parts], axis=1)


def fetch(sem, *pairs):
    copies = [pltpu.make_async_copy(source, target, sem.at[i]) for i, (source, target) in enumerate(pairs)]
    for copy in copies:
        copy.start()
    return copies


def lay_out(rows, distances, own_ref, other_ref, halo_ref, z_ref, e_ref, f_ref):
    core = lax.rem(lax.axis_index("height"), 2)
    slots = 3 * rows
    per = COLS // SEG
    high = rows + 2

    frames = range(2 * distances[0], 6)
    for frame in frames:
        for slot in (0, slots - 1):
            row = (frame * slots + slot) * SEG
            for half in range(2):
                z_ref[half, row : row + SEG, :] = jnp.zeros((SEG, LANES), F32)

    def spread(piece, frame, slot):
        base = pl.multiple_of((frame * slots + slot) * SEG, SEG)
        count = piece.shape[0]
        edge = jnp.zeros((count, LANES), F32)
        wide = jnp.concatenate([edge, piece, edge, edge], axis=1)
        for s in range(SEG):
            for half in range(2):
                start = LANES + s * per * C_IN - C_IN + half * 6 * C_IN
                lo = start // LANES * LANES
                window = wide[:, lo : lo + 2 * LANES]
                if start > lo:
                    window = pltpu.roll(window, 2 * LANES - (start - lo), 1)
                z_ref[half, pl.ds(base + s, count, stride=SEG), :] = window[:, :LANES]

    main = jnp.where(core == 0, rows, 0)
    edge_slot = jnp.where(core == 0, rows - 2, 2 * rows)
    row_block, last_block = lax.axis_index("height"), lax.axis_size("height") - 1
    beside = jnp.where(core == 0, row_block > 0, row_block < last_block)
    for d in distances:
        real = lax.axis_index("tm") >= 2 - d

        def piece(ref, keep, *index):
            return jnp.where(keep, ref[(*index, d)].astype(F32), 0.0)

        spread(piece(own_ref, real), 2 * d + core, main)
        spread(piece(other_ref, real), 2 * d + 1 - core, main)
        spread(piece(halo_ref, real & beside, 0), 2 * d + core, edge_slot)
        spread(piece(halo_ref, real & beside, 1), 2 * d + 1 - core, edge_slot)

    first = rows - 2
    span = rows + 4
    low_side = lax.broadcasted_iota(jnp.int32, (span * SEG, LANES), 1) < LANES // 2
    where = [(0, 0), (0, 2 * C_IN), (0, 4 * C_IN), (1, 0), (1, 2 * C_IN)]

    def turned(x, shift):
        return x if shift % LANES == 0 else pltpu.roll(x, shift % LANES, 1)

    for pair, (half, offset) in enumerate(where):
        upper = []
        for frame in frames:
            x = z_ref[half, pl.ds((frame * slots + first) * SEG, (span + 1) * SEG), :]
            low, up = turned(x, -offset), turned(x, LANES // 2 - offset)
            e_ref[pair, frame] = jnp.where(low_side, low[: span * SEG], up[SEG:]).astype(BF16)
            if frames[0] < frame < 5:
                f_ref[pair, frame - 1] = jnp.where(
                    low_side[: high * SEG], upper, up[2 * SEG : span * SEG]
                ).astype(BF16)
            upper = low[2 * SEG : span * SEG]


def exact_product(rows, member):
    parts = []
    for x in rows:
        for _ in range(3):
            part = x.astype(BF16).astype(F32)
            parts.append(part)
            x = x - part
    parts.append(jnp.zeros((16 - len(parts), x.shape[1]), F32))
    out = jnp.dot(jnp.concatenate(parts, axis=0).astype(BF16), member.astype(BF16), preferred_element_type=F32)
    return [out[3 * i : 3 * i + 1] + out[3 * i + 1 : 3 * i + 2] + out[3 * i + 2 : 3 * i + 3] for i in range(len(rows))]


def stats_kernel(rows, own_ref, other_ref, halo_ref, band_ref, v_ref, sum_ref, z_ref, e_ref, f_ref):
    lay_out(rows, (1, 2), own_ref, other_ref, halo_ref, z_ref, e_ref, f_ref)
    channels = v_ref.shape[1]
    per = COLS // SEG
    sums = jnp.zeros((8, 2 * channels), F32)
    squares = jnp.zeros((8, 2 * channels), F32)
    bias = jnp.concatenate([v_ref[0:1, :], v_ref[0:1, :]], axis=1)
    for pair in range(per // 2):
        out = jnp.dot(
            windows(e_ref, f_ref, pair, (2, 4), (1, 1 + rows)), band_ref[...], preferred_element_type=F32
        )
        out = (out + bias).reshape(-1, 8, 2 * channels)
        sums = sums + jnp.sum(out, axis=0)
        squares = squares + jnp.sum(out * out, axis=0)
    whole = []
    for part in (sums, squares):
        row = jnp.sum(part, axis=0, keepdims=True)
        whole.append(row[:, :channels] + row[:, channels:])
    size = channels // GROUPS
    row = lax.broadcasted_iota(jnp.int32, (channels, LANES), 0)
    first = lax.rem(lax.broadcasted_iota(jnp.int32, (channels, LANES), 1), GROUPS) * size
    member = jnp.where((row >= first) & (row < first + size), 1.0, 0.0)
    per_group = exact_product(whole, member)
    lane = lax.broadcasted_iota(jnp.int32, (1, LANES), 1)
    payload = jnp.where(lane < GROUPS, per_group[0], per_group[1])
    sum_ref[:, 0, :] = jnp.broadcast_to(payload, (sum_ref.shape[0], LANES))


def opened_kernel(
    rows, own_ref, other_ref, halo_ref, band_ref, v_ref, first_ref, o_hbm, z_ref, e_ref, f_ref, o_ref, sem
):
    lay_out(rows, (0, 1, 2), own_ref, other_ref, halo_ref, z_ref, e_ref, f_ref)
    channels = v_ref.shape[1]
    high = rows + 2
    stores = []
    for t0, t1 in ((2, 4), (1, 2), (0, 1)):
        here = pl.ds(t0 - 1, t1 - t0)
        for pair in range(COLS // SEG // 2):
            lhs = windows(e_ref, f_ref, pair, (t0, t1), (0, high))
            out = jnp.dot(lhs, band_ref[...], preferred_element_type=F32)
            for e in range(2):
                part = out[:, e * channels : (e + 1) * channels] + v_ref[0:1, :]
                part = part.reshape(t1 - t0, high, SEG, channels)
                if t0:
                    o_ref[here, :, 2 * pair + e] = part
                else:
                    first_ref[:, 2 * pair + e] = part[0]
        if t0:
            stores += fetch(sem.at[t0 - 1], (o_ref.at[here], o_hbm.at[here]))
    for store in stores:
        store.wait()


def second_kernel(
    rows, entries, sum_ref, first_ref, o_hbm, head_ref, w_hbm, v_ref, out_hbm,
    a_ref, place_ref, main_ref, two_ref, w_ref, o_ref, out_ref, sem,
):
    channels = v_ref.shape[1]
    per = COLS // SEG
    high = rows + 2
    third = 3 * channels
    weights = [
        pltpu.make_async_copy(w_hbm.at[pl.ds(i * third, third)], w_ref.at[pl.ds((i - 2) * third, third)], sem.at[i])
        for i in range(2, 9)
    ]
    loads = [pltpu.make_async_copy(o_hbm.at[t], o_ref.at[t], sem.at[9 + t]) for t in range(3)]
    for copy in (loads[0], *weights[:4], loads[1], *weights[4:], loads[2]):
        copy.start()
    height = lax.axis_index("height")
    frame = lax.axis_index("tm")
    size = channels // GROUPS
    lane = lax.broadcasted_iota(jnp.int32, (1, LANES), 1)
    total = jnp.sum(sum_ref[:, 0, :], axis=0, keepdims=True)
    mean = total / entries
    var = pltpu.roll(mean, LANES - GROUPS, 1) - mean * mean
    inverse = lax.rsqrt(jnp.where(lane < GROUPS, var, 1.0) + 1e-06)
    first = lax.broadcasted_iota(jnp.int32, (LANES, channels), 0) * size
    column = lax.broadcasted_iota(jnp.int32, (LANES, channels), 1)
    member = jnp.where((column >= first) & (column < first + size), 1.0, 0.0)
    mean, inverse = exact_product([mean, inverse], member)
    scale = inverse * v_ref[1:2, :]
    half_scale = 0.5 * scale
    half_shift = 0.5 * (v_ref[2:3, :] - mean * scale)
    lane_row = lax.broadcasted_iota(jnp.int32, (SEG, channels), 0)

    def act_rows(t):
        return [functools.partial(act, t, h) for h in range(high)]

    def act(t, *hs):
        for h in hs or range(high):
            row = height * rows - 1 + h
            inside = (frame * FR_DEV - 2 + t >= 0) & (row >= 0) & (row < rows * lax.axis_size("height"))
            x = o_ref[t - 1, h] if t else first_ref[h]
            u = x.reshape(per * SEG, channels) * half_scale + half_shift
            y = u + u * jnp.tanh(u)
            y = jnp.where(inside, y, 0.0)
            a_ref[t, h, 1 : per + 1] = y.astype(BF16).reshape(per, SEG, channels)
            before = jnp.where(lane_row == 0, 0.0, pltpu.roll(y[(per - 1) * SEG :], 1, 0))
            after = jnp.where(lane_row == SEG - 1, 0.0, pltpu.roll(y[:SEG], SEG - 1, 0))
            a_ref[t, h, 0] = before.astype(BF16)
            a_ref[t, h, per + 1] = after.astype(BF16)

    wide = channels // (2 * LANES) * 2 * LANES

    def patch(frame, b, c, count):
        return a_ref[frame, b : b + rows, c : c + count].reshape(rows * count * SEG, channels)

    def tap(a, b, c, lanes):
        row = ((a * 3 + b) * 3 + c) * channels
        if row < head_ref.shape[0]:
            return head_ref[row : row + channels, lanes]
        row -= head_ref.shape[0]
        return w_ref[row : row + channels, lanes]

    def product(pairs, beside=()):
        beside = list(beside)
        acc = None
        for i in range(0, len(pairs), 2):
            some = pairs[i : i + 2]
            lhs = jnp.concatenate([x() for x, _ in some], axis=1)
            rhs = jnp.concatenate([y() for _, y in some], axis=0)
            part = jnp.dot(lhs, rhs, preferred_element_type=F32)
            acc = part if acc is None else acc + part
            if beside:
                beside.pop(0)()
        for step in beside:
            step()
        return acc

    low, rest = slice(0, wide), slice(wide, channels)

    def edge(t, a, start):
        f = t + a
        for i, (bs, beside) in enumerate(start):
            parts = (
                product([
                    (functools.partial(patch, f, b, c, per), functools.partial(tap, a, b, c, low))
                    for b in bs for c in range(3)
                ], beside),
                product([
                    (
                        functools.partial(patch, f, b, 0, per + 1),
                        lambda b=b: jnp.concatenate([tap(a, b, 0, rest), tap(a, b, 1, rest)], axis=1),
                    )
                    for b in bs
                ]),
                product([
                    (functools.partial(patch, f, b, 2, per), functools.partial(tap, a, b, 2, rest)) for b in bs
                ]),
            )
            if i == 0 and a == 0:
                main_ref[t, :, low], two_ref[t], main_ref[t, :, rest] = parts
            elif i == 0:
                two_ref[t] = parts[1]
                main_ref[t, :, low] += parts[0]
                main_ref[t, :, rest] += parts[2]
            else:
                two_ref[t] += parts[1]
                main_ref[t, :, low] += parts[0]
                main_ref[t, :, rest] += parts[2]

    def shared(f, beside):
        whole = slice(0, channels)
        both = product([
            (
                functools.partial(patch, f, b, c, per),
                lambda b=b, c=c: jnp.concatenate([tap(f, b, c, whole), tap(f - 1, b, c, whole)], axis=1),
            )
            for b in range(3) for c in range(3)
        ], beside)
        main_ref[0] += both[:, :channels]
        if f == 1:
            main_ref[1] = both[:, channels:]
        else:
            main_ref[1] += both[:, channels:]

    def finish(t):
        two = two_ref[t].reshape(rows, per + 1, SEG, 2 * LANES)
        size = rows * per * SEG
        main = main_ref[t, :, low]
        one = main_ref[t, :, rest]
        one = one + two[:, :per, :, :LANES].reshape(size, LANES) + two[:, 1:, :, LANES:].reshape(size, LANES)
        for h in range(rows):
            base = h * per * SEG
            opened = o_ref[t + 1, h + 1].reshape(per * SEG, channels)
            for tile in range(channels // LANES):
                lanes = slice(tile * LANES, (tile + 1) * LANES)
                source = main[:, lanes] if tile * LANES < wide else one
                whole = source[base : base + per * SEG] + v_ref[3:4, lanes] + opened[:, lanes]
                for k in range(per):
                    place_ref[t, h, tile, pl.ds(k, SEG, stride=per), :] = whole[k * SEG : (k + 1) * SEG]
                out_ref[t, h, :, lanes] = place_ref[t, h, tile].astype(BF16)
        store = pltpu.make_async_copy(out_ref.at[t], out_hbm.at[t], sem.at[14 + t])
        store.start()
        return store

    def need(*copies):
        for copy in copies:
            copy.wait()

    def steps(*parts):
        return [lambda group=group: [step() for step in group] for group in parts]

    rows1, rows2, rows3 = (act_rows(t) for t in (1, 2, 3))
    act(0)
    wait1 = functools.partial(need, weights[0], loads[0])
    wait2 = functools.partial(need, *weights[1:4])
    arrived = functools.partial(need, loads[1])
    wait3 = functools.partial(need, *weights[4:], loads[2])
    wait3a = functools.partial(need, *weights[4:])
    wait3b = functools.partial(need, loads[2])
    edge(0, 0, [((0, 1), steps([], [], [wait1])), ((2,), steps(rows1, [wait2]))])
    shared(1, steps([], [arrived, wait3], rows2))
    shared(2, steps(rows3))
    first = finish(0)
    edge(1, 2, [((0, 1, 2), [])])
    second = finish(1)
    need(first, second)


def second_part(rows, entries, sums, first, opened, head, weight, vectors):
    high, per, channels, frames = rows + 2, COLS // SEG, vectors.shape[1], FR_DEV
    vmem, hbm = pl.BlockSpec(memory_space=pltpu.VMEM), pl.BlockSpec(memory_space=pltpu.HBM)
    size = rows * per * SEG
    out_shape = (frames, rows, COLS, channels)
    return pl.pallas_call(
        functools.partial(second_kernel, rows, entries),
        out_shape=pltpu.HBM(out_shape, BF16),
        in_specs=[vmem, vmem, hbm, vmem, hbm, vmem],
        out_specs=hbm,
        scratch_shapes=[
            pltpu.VMEM((4, high, per + 2, SEG, channels), BF16),
            pltpu.VMEM((frames, rows, channels // LANES, COLS, LANES), F32),
            pltpu.VMEM((frames, size, channels), F32),
            pltpu.VMEM((frames, size // per * (per + 1), 2 * LANES), F32),
            pltpu.VMEM((weight.shape[0] - head.shape[0], channels), BF16),
            pltpu.VMEM(opened.shape, F32),
            pltpu.VMEM(out_shape, BF16),
            pltpu.SemaphoreType.DMA((16,)),
        ],
        compiler_params=pltpu.CompilerParams(vmem_limit_bytes=36 << 20),
        name="second",
    )(sums, first, opened, head, weight, vectors)


def shards(latent, in_weight, in_bias, norm_gain, norm_bias, conv_weight, conv_bias):
    frames = FR_DEV
    rows = latent.shape[0] // frames
    channels = conv_weight.shape[1]
    tm, height = lax.axis_size("tm"), lax.axis_size("height")
    half = height // 2
    core = lax.axis_index("height") % 2
    band, vectors = pl.pallas_call(
        band_kernel,
        out_shape=(
            pltpu.VMEM((5 * LANES, 2 * channels), BF16),
            pltpu.VMEM((4, channels), F32),
        ),
        name="band",
    )(in_weight, in_bias, norm_gain, norm_bias, conv_bias)

    received = []
    for d in (2, 1, 0):
        route = [
            (i * height + p * half + m, (i + d) % tm * height + 2 * m + p)
            for i in range(tm)
            for p in range(2)
            for m in range(half)
        ]
        received.append(lax.ppermute(latent, ("tm", "height"), route))
    own = jnp.stack(received)
    other = lax.ppermute(own, "height", [(i, i ^ 1) for i in range(height)])
    edge = lax.dynamic_slice_in_dim(jnp.stack([own, other]), (1 - core) * (2 * rows - 2), 2, axis=2)
    down = [(2 * m, 2 * m + 2) for m in range(half - 1)] + [(height - 2, height - 1)]
    up = [(2 * m + 1, 2 * m - 1) for m in range(1, half)] + [(1, 0)]
    halo = lax.ppermute(edge, "height", down + up)

    per = COLS // SEG
    high = rows + 2
    vmem, hbm = pl.BlockSpec(memory_space=pltpu.VMEM), pl.BlockSpec(memory_space=pltpu.HBM)

    def keep(x):
        return pltpu.with_memory_space_constraint(x, pltpu.HBM)

    scratch = [
        pltpu.VMEM((2, 6 * 3 * rows * SEG, LANES), F32),
        pltpu.VMEM((per // 2, 6, (rows + 4) * SEG, LANES), BF16),
        pltpu.VMEM((per // 2, 4, high * SEG, LANES), BF16),
    ]
    sums = pl.pallas_call(
        functools.partial(stats_kernel, rows),
        out_shape=jax.ShapeDtypeStruct((tm * height, 1, LANES), F32),
        in_specs=[vmem] * 5,
        scratch_shapes=scratch,
        compiler_params=pltpu.CompilerParams(vmem_limit_bytes=12 << 20),
        name="stats",
    )(own, other, halo, band, vectors)
    sums, later_weight = lax.optimization_barrier((sums, conv_weight))
    sums = lax.all_to_all(sums, ("tm", "height"), 0, 0, tiled=True)
    positions = 4 * high * per * SEG
    opened_shape = (3, high, per, SEG, channels)
    first, opened = pl.pallas_call(
        functools.partial(opened_kernel, rows),
        out_shape=(pltpu.VMEM(opened_shape[1:], F32), pltpu.HBM(opened_shape, F32)),
        in_specs=[vmem] * 5,
        out_specs=(vmem, hbm),
        scratch_shapes=[*scratch, pltpu.VMEM(opened_shape, F32), pltpu.SemaphoreType.DMA((2, 1))],
        cost_estimate=pl.CostEstimate(
            flops=2 * positions * 5 * LANES * channels, transcendentals=0, bytes_accessed=4 * positions * channels
        ),
        compiler_params=pltpu.CompilerParams(vmem_limit_bytes=16 << 20),
        name="opened",
    )(own, other, halo, band, vectors)
    entries = frames * tm * rows * height * COLS * (channels // GROUPS)
    head = pltpu.with_memory_space_constraint(later_weight[: 6 * channels], pltpu.VMEM)
    return second_part(rows, entries, sums, first, keep(opened), head, keep(conv_weight), vectors)


def solution(mesh):
    return jax.shard_map(
        shards,
        mesh=mesh,
        in_specs=(P(("tm", "height"), None), P(), P(), P(), P(), P(), P()),
        out_specs=P("tm", "height", None, None),
        check_vma=False,
    )
```

```python
import functools

import jax
import jax.numpy as jnp
from jax import lax
from jax.experimental import pallas as pl
from jax.experimental.pallas import tpu as pltpu
from jax.sharding import PartitionSpec as P

C_IN = 16
GROUPS = 32
COLS = 160
FR_DEV = 2
SEG = 16
LANES = 128
F32 = jnp.float32
BF16 = jnp.bfloat16


def band_kernel(w_ref, *refs):
    *vectors, o_ref, v_ref = refs
    for i, vector in enumerate(vectors):
        v_ref[i : i + 1, :] = vector[...].reshape(1, -1)
    o_ref[...] = jnp.zeros_like(o_ref)
    channels = w_ref.shape[1]
    depth = 3 * C_IN
    places = [(a, b, a, b) for a in range(3) for b in range(2)] + [(0, 2, 3, 0), (1, 2, 3, 1), (2, 2, 4, 0)]
    for a, b, group, side in places:
        for e in range(2):
            row = group * LANES + side * (LANES // 2) + e * C_IN
            tap = (a * 3 + b) * depth
            o_ref[row : row + depth, e * channels : (e + 1) * channels] = w_ref[tap : tap + depth, :]


def windows(e_ref, f_ref, pair, frames, high):
    (t0, t1), (h0, h1) = frames, high
    rows = slice(h0 * SEG, h1 * SEG)
    parts = [e_ref[pair, t0 + a : t1 + a, rows] for a in range(3)]
    parts.append(f_ref[pair, t0:t1, rows])
    parts.append(e_ref[pair, t0 + 2 : t1 + 2, (h0 + 2) * SEG : (h1 + 2) * SEG])
    size = (t1 - t0) * (h1 - h0) * SEG
    return jnp.concatenate([part.reshape(size, LANES) for part in parts], axis=1)


def fetch(sem, *pairs):
    copies = [pltpu.make_async_copy(source, target, sem.at[i]) for i, (source, target) in enumerate(pairs)]
    for copy in copies:
        copy.start()
    return copies


def lay_out(rows, distances, own_ref, other_ref, halo_ref, z_ref, e_ref, f_ref):
    core = lax.rem(lax.axis_index("height"), 2)
    slots = 3 * rows
    per = COLS // SEG
    high = rows + 2

    frames = range(2 * distances[0], 6)
    for frame in frames:
        for slot in (0, slots - 1):
            row = (frame * slots + slot) * SEG
            for half in range(2):
                z_ref[half, row : row + SEG, :] = jnp.zeros((SEG, LANES), F32)

    def spread(piece, frame, *places):
        edge = jnp.zeros((piece.shape[0], LANES), F32)
        wide = jnp.concatenate([edge, piece, edge, edge], axis=1)
        for s in range(SEG):
            for half in range(2):
                start = LANES + s * per * C_IN - C_IN + half * 6 * C_IN
                lo = start // LANES * LANES
                window = wide[:, lo : lo + 2 * LANES]
                if start > lo:
                    window = pltpu.roll(window, 2 * LANES - (start - lo), 1)
                done = 0
                for count, slot in places:
                    base = pl.multiple_of((frame * slots + slot) * SEG, SEG)
                    z_ref[half, pl.ds(base + s, count, stride=SEG), :] = window[done : done + count, :LANES]
                    done += count

    main = jnp.where(core == 0, rows, 0)
    edge_slot = jnp.where(core == 0, rows - 2, 2 * rows)
    row_block, last_block = lax.axis_index("height"), lax.axis_size("height") - 1
    beside = jnp.where(core == 0, row_block > 0, row_block < last_block)
    for d in distances:
        real = lax.axis_index("tm") >= 2 - d

        def piece(ref, keep, *index):
            return jnp.where(keep, ref[(*index, d)].astype(F32), 0.0)

        places = ((2 * rows, main), (2, edge_slot))
        for ref, side, frame in ((own_ref, 0, 2 * d + core), (other_ref, 1, 2 * d + 1 - core)):
            both = jnp.concatenate([piece(ref, real), piece(halo_ref, real & beside, side)], axis=0)
            spread(both, frame, *places)

    first = rows - 2
    span = rows + 4
    low_side = lax.broadcasted_iota(jnp.int32, (span * SEG, LANES), 1) < LANES // 2
    where = [(0, 0), (0, 2 * C_IN), (0, 4 * C_IN), (1, 0), (1, 2 * C_IN)]

    def turned(x, shift):
        return x if shift % LANES == 0 else pltpu.roll(x, shift % LANES, 1)

    for pair, (half, offset) in enumerate(where):
        upper = []
        for frame in frames:
            x = z_ref[half, pl.ds((frame * slots + first) * SEG, (span + 1) * SEG), :]
            low, up = turned(x, -offset), turned(x, LANES // 2 - offset)
            e_ref[pair, frame] = jnp.where(low_side, low[: span * SEG], up[SEG:]).astype(BF16)
            if frames[0] < frame < 5:
                f_ref[pair, frame - 1] = jnp.where(
                    low_side[: high * SEG], upper, up[2 * SEG : span * SEG]
                ).astype(BF16)
            upper = low[2 * SEG : span * SEG]


def exact_product(rows, member):
    parts = []
    for x in rows:
        for _ in range(3):
            part = x.astype(BF16).astype(F32)
            parts.append(part)
            x = x - part
    parts.append(jnp.zeros((16 - len(parts), x.shape[1]), F32))
    out = jnp.dot(jnp.concatenate(parts, axis=0).astype(BF16), member.astype(BF16), preferred_element_type=F32)
    return [out[3 * i : 3 * i + 1] + out[3 * i + 1 : 3 * i + 2] + out[3 * i + 2 : 3 * i + 3] for i in range(len(rows))]


def stats_kernel(rows, own_ref, other_ref, halo_ref, band_ref, v_ref, sum_ref, z_ref, e_ref, f_ref):
    lay_out(rows, (1, 2), own_ref, other_ref, halo_ref, z_ref, e_ref, f_ref)
    channels = v_ref.shape[1]
    per = COLS // SEG
    sums = jnp.zeros((8, 2 * channels), F32)
    squares = jnp.zeros((8, 2 * channels), F32)
    bias = jnp.concatenate([v_ref[0:1, :], v_ref[0:1, :]], axis=1)
    for pair in range(per // 2):
        out = jnp.dot(
            windows(e_ref, f_ref, pair, (2, 4), (1, 1 + rows)), band_ref[...], preferred_element_type=F32
        )
        out = (out + bias).reshape(-1, 8, 2 * channels)
        sums = sums + jnp.sum(out, axis=0)
        squares = squares + jnp.sum(out * out, axis=0)
    whole = []
    for part in (sums, squares):
        row = jnp.sum(part, axis=0, keepdims=True)
        whole.append(row[:, :channels] + row[:, channels:])
    size = channels // GROUPS
    row = lax.broadcasted_iota(jnp.int32, (channels, LANES), 0)
    first = lax.rem(lax.broadcasted_iota(jnp.int32, (channels, LANES), 1), GROUPS) * size
    member = jnp.where((row >= first) & (row < first + size), 1.0, 0.0)
    per_group = exact_product(whole, member)
    lane = lax.broadcasted_iota(jnp.int32, (1, LANES), 1)
    payload = jnp.where(lane < GROUPS, per_group[0], per_group[1])
    sum_ref[:, 0, :] = jnp.broadcast_to(payload, (sum_ref.shape[0], LANES))


def opened_kernel(
    rows, own_ref, other_ref, halo_ref, band_ref, v_ref, first_ref, o_hbm, z_ref, e_ref, f_ref, o_ref, sem
):
    lay_out(rows, (0, 1, 2), own_ref, other_ref, halo_ref, z_ref, e_ref, f_ref)
    channels = v_ref.shape[1]
    high = rows + 2
    stores = []
    for t0, t1 in ((2, 4), (1, 2), (0, 1)):
        here = pl.ds(t0 - 1, t1 - t0)
        for pair in range(COLS // SEG // 2):
            lhs = windows(e_ref, f_ref, pair, (t0, t1), (0, high))
            out = jnp.dot(lhs, band_ref[...], preferred_element_type=F32)
            for e in range(2):
                part = out[:, e * channels : (e + 1) * channels] + v_ref[0:1, :]
                part = part.reshape(t1 - t0, high, SEG, channels)
                if t0:
                    o_ref[here, :, 2 * pair + e] = part
                else:
                    first_ref[:, 2 * pair + e] = part[0]
        if t0:
            stores += fetch(sem.at[t0 - 1], (o_ref.at[here], o_hbm.at[here]))
    for store in stores:
        store.wait()


def second_kernel(
    rows, entries, sum_ref, first_ref, o_hbm, head_ref, w_hbm, v_ref, out_hbm,
    a_ref, place_ref, main_ref, two_ref, w_ref, o_ref, out_ref, sem,
):
    channels = v_ref.shape[1]
    per = COLS // SEG
    high = rows + 2
    third = 3 * channels
    weights = [
        pltpu.make_async_copy(w_hbm.at[pl.ds(i * third, third)], w_ref.at[pl.ds((i - 2) * third, third)], sem.at[i])
        for i in range(2, 9)
    ]
    loads = [pltpu.make_async_copy(o_hbm.at[t], o_ref.at[t], sem.at[9 + t]) for t in range(3)]
    for copy in (loads[0], *weights[:4], loads[1], *weights[4:], loads[2]):
        copy.start()
    height = lax.axis_index("height")
    frame = lax.axis_index("tm")
    size = channels // GROUPS
    lane = lax.broadcasted_iota(jnp.int32, (1, LANES), 1)
    total = jnp.sum(sum_ref[:, 0, :], axis=0, keepdims=True)
    mean = total / entries
    var = pltpu.roll(mean, LANES - GROUPS, 1) - mean * mean
    inverse = lax.rsqrt(jnp.where(lane < GROUPS, var, 1.0) + 1e-06)
    first = lax.broadcasted_iota(jnp.int32, (LANES, channels), 0) * size
    column = lax.broadcasted_iota(jnp.int32, (LANES, channels), 1)
    member = jnp.where((column >= first) & (column < first + size), 1.0, 0.0)
    mean, inverse = exact_product([mean, inverse], member)
    scale = inverse * v_ref[1:2, :]
    half_scale = 0.5 * scale
    half_shift = 0.5 * (v_ref[2:3, :] - mean * scale)
    lane_row = lax.broadcasted_iota(jnp.int32, (SEG, channels), 0)

    def act_rows(t):
        return [functools.partial(act, t, h) for h in range(high)]

    def act(t, *hs):
        for h in hs or range(high):
            row = height * rows - 1 + h
            inside = (frame * FR_DEV - 2 + t >= 0) & (row >= 0) & (row < rows * lax.axis_size("height"))
            x = o_ref[t - 1, h] if t else first_ref[h]
            u = x.reshape(per * SEG, channels) * half_scale + half_shift
            y = u + u * jnp.tanh(u)
            y = jnp.where(inside, y, 0.0)
            a_ref[t, h, 1 : per + 1] = y.astype(BF16).reshape(per, SEG, channels)
            before = jnp.where(lane_row == 0, 0.0, pltpu.roll(y[(per - 1) * SEG :], 1, 0))
            after = jnp.where(lane_row == SEG - 1, 0.0, pltpu.roll(y[:SEG], SEG - 1, 0))
            a_ref[t, h, 0] = before.astype(BF16)
            a_ref[t, h, per + 1] = after.astype(BF16)

    wide = channels // (2 * LANES) * 2 * LANES

    def patch(frame, b, c, count):
        return a_ref[frame, b : b + rows, c : c + count].reshape(rows * count * SEG, channels)

    def tap(a, b, c, lanes):
        row = ((a * 3 + b) * 3 + c) * channels
        if row < head_ref.shape[0]:
            return head_ref[row : row + channels, lanes]
        row -= head_ref.shape[0]
        return w_ref[row : row + channels, lanes]

    def product(pairs, beside=()):
        beside = list(beside)
        acc = None
        for i in range(0, len(pairs), 2):
            some = pairs[i : i + 2]
            lhs = jnp.concatenate([x() for x, _ in some], axis=1)
            rhs = jnp.concatenate([y() for _, y in some], axis=0)
            part = jnp.dot(lhs, rhs, preferred_element_type=F32)
            acc = part if acc is None else acc + part
            if beside:
                beside.pop(0)()
        for step in beside:
            step()
        return acc

    low, rest = slice(0, wide), slice(wide, channels)

    def edge(t, a, start):
        f = t + a
        for i, (bs, beside) in enumerate(start):
            parts = (
                product([
                    (functools.partial(patch, f, b, c, per), functools.partial(tap, a, b, c, low))
                    for b in bs for c in range(3)
                ], beside),
                product([
                    (
                        functools.partial(patch, f, b, 0, per + 1),
                        lambda b=b: jnp.concatenate([tap(a, b, 0, rest), tap(a, b, 1, rest)], axis=1),
                    )
                    for b in bs
                ]),
                product([
                    (functools.partial(patch, f, b, 2, per), functools.partial(tap, a, b, 2, rest)) for b in bs
                ]),
            )
            if i == 0 and a == 0:
                main_ref[t, :, low], two_ref[t], main_ref[t, :, rest] = parts
            elif i == 0:
                two_ref[t] = parts[1]
                main_ref[t, :, low] += parts[0]
                main_ref[t, :, rest] += parts[2]
            else:
                two_ref[t] += parts[1]
                main_ref[t, :, low] += parts[0]
                main_ref[t, :, rest] += parts[2]

    def shared(f, beside):
        whole = slice(0, channels)
        both = product([
            (
                functools.partial(patch, f, b, c, per),
                lambda b=b, c=c: jnp.concatenate([tap(f, b, c, whole), tap(f - 1, b, c, whole)], axis=1),
            )
            for b in range(3) for c in range(3)
        ], beside)
        main_ref[0] += both[:, :channels]
        if f == 1:
            main_ref[1] = both[:, channels:]
        else:
            main_ref[1] += both[:, channels:]

    def finish(t):
        two = two_ref[t].reshape(rows, per + 1, SEG, 2 * LANES)
        size = rows * per * SEG
        main = main_ref[t, :, low]
        one = main_ref[t, :, rest]
        one = one + two[:, :per, :, :LANES].reshape(size, LANES) + two[:, 1:, :, LANES:].reshape(size, LANES)
        for h in range(rows):
            base = h * per * SEG
            opened = o_ref[t + 1, h + 1].reshape(per * SEG, channels)
            for tile in range(channels // LANES):
                lanes = slice(tile * LANES, (tile + 1) * LANES)
                source = main[:, lanes] if tile * LANES < wide else one
                whole = source[base : base + per * SEG] + v_ref[3:4, lanes] + opened[:, lanes]
                for k in range(per):
                    place_ref[t, h, tile, pl.ds(k, SEG, stride=per), :] = whole[k * SEG : (k + 1) * SEG]
                out_ref[t, h, :, lanes] = place_ref[t, h, tile].astype(BF16)
        store = pltpu.make_async_copy(out_ref.at[t], out_hbm.at[t], sem.at[14 + t])
        store.start()
        return store

    def need(*copies):
        for copy in copies:
            copy.wait()

    def steps(*parts):
        return [lambda group=group: [step() for step in group] for group in parts]

    rows1, rows2, rows3 = (act_rows(t) for t in (1, 2, 3))
    act(0)
    wait1 = functools.partial(need, weights[0], loads[0])
    wait2 = functools.partial(need, *weights[1:4], loads[1])
    wait3 = functools.partial(need, *weights[4:], loads[2])
    wait3a = functools.partial(need, *weights[4:])
    wait3b = functools.partial(need, loads[2])
    edge(0, 0, [((0, 1), steps([], [], [wait1])), ((2,), steps(rows1, [wait2]))])
    shared(1, steps(rows2, [wait3]))
    shared(2, steps(rows3))
    first = finish(0)
    edge(1, 2, [((0, 1, 2), [])])
    second = finish(1)
    need(first, second)


def second_part(rows, entries, sums, first, opened, head, weight, vectors):
    high, per, channels, frames = rows + 2, COLS // SEG, vectors.shape[1], FR_DEV
    vmem, hbm = pl.BlockSpec(memory_space=pltpu.VMEM), pl.BlockSpec(memory_space=pltpu.HBM)
    size = rows * per * SEG
    out_shape = (frames, rows, COLS, channels)
    return pl.pallas_call(
        functools.partial(second_kernel, rows, entries),
        out_shape=pltpu.HBM(out_shape, BF16),
        in_specs=[vmem, vmem, hbm, vmem, hbm, vmem],
        out_specs=hbm,
        scratch_shapes=[
            pltpu.VMEM((4, high, per + 2, SEG, channels), BF16),
            pltpu.VMEM((frames, rows, channels // LANES, COLS, LANES), F32),
            pltpu.VMEM((frames, size, channels), F32),
            pltpu.VMEM((frames, size // per * (per + 1), 2 * LANES), F32),
            pltpu.VMEM((weight.shape[0] - head.shape[0], channels), BF16),
            pltpu.VMEM(opened.shape, F32),
            pltpu.VMEM(out_shape, BF16),
            pltpu.SemaphoreType.DMA((16,)),
        ],
        compiler_params=pltpu.CompilerParams(vmem_limit_bytes=36 << 20),
        name="second",
    )(sums, first, opened, head, weight, vectors)


def shards(latent, in_weight, in_bias, norm_gain, norm_bias, conv_weight, conv_bias):
    frames = FR_DEV
    rows = latent.shape[0] // frames
    channels = conv_weight.shape[1]
    tm, height = lax.axis_size("tm"), lax.axis_size("height")
    half = height // 2
    core = lax.axis_index("height") % 2
    band, vectors = pl.pallas_call(
        band_kernel,
        out_shape=(
            pltpu.VMEM((5 * LANES, 2 * channels), BF16),
            pltpu.VMEM((4, channels), F32),
        ),
        name="band",
    )(in_weight, in_bias, norm_gain, norm_bias, conv_bias)

    received = []
    for d in (2, 1, 0):
        route = [
            (i * height + p * half + m, (i + d) % tm * height + 2 * m + p)
            for i in range(tm)
            for p in range(2)
            for m in range(half)
        ]
        received.append(lax.ppermute(latent, ("tm", "height"), route))
    own = jnp.stack(received)
    other = lax.ppermute(own, "height", [(i, i ^ 1) for i in range(height)])
    edge = lax.dynamic_slice_in_dim(jnp.stack([own, other]), (1 - core) * (2 * rows - 2), 2, axis=2)
    down = [(2 * m, 2 * m + 2) for m in range(half - 1)] + [(height - 2, height - 1)]
    up = [(2 * m + 1, 2 * m - 1) for m in range(1, half)] + [(1, 0)]
    halo = lax.ppermute(edge, "height", down + up)

    per = COLS // SEG
    high = rows + 2
    vmem, hbm = pl.BlockSpec(memory_space=pltpu.VMEM), pl.BlockSpec(memory_space=pltpu.HBM)

    def keep(x):
        return pltpu.with_memory_space_constraint(x, pltpu.HBM)

    scratch = [
        pltpu.VMEM((2, 6 * 3 * rows * SEG, LANES), F32),
        pltpu.VMEM((per // 2, 6, (rows + 4) * SEG, LANES), BF16),
        pltpu.VMEM((per // 2, 4, high * SEG, LANES), BF16),
    ]
    sums = pl.pallas_call(
        functools.partial(stats_kernel, rows),
        out_shape=jax.ShapeDtypeStruct((tm * height, 1, LANES), F32),
        in_specs=[vmem] * 5,
        scratch_shapes=scratch,
        compiler_params=pltpu.CompilerParams(vmem_limit_bytes=12 << 20),
        name="stats",
    )(own, other, halo, band, vectors)
    sums, later_weight = lax.optimization_barrier((sums, conv_weight))
    sums = lax.all_to_all(sums, ("tm", "height"), 0, 0, tiled=True)
    positions = 4 * high * per * SEG
    opened_shape = (3, high, per, SEG, channels)
    first, opened = pl.pallas_call(
        functools.partial(opened_kernel, rows),
        out_shape=(pltpu.VMEM(opened_shape[1:], F32), pltpu.HBM(opened_shape, F32)),
        in_specs=[vmem] * 5,
        out_specs=(vmem, hbm),
        scratch_shapes=[*scratch, pltpu.VMEM(opened_shape, F32), pltpu.SemaphoreType.DMA((2, 1))],
        cost_estimate=pl.CostEstimate(
            flops=2 * positions * 5 * LANES * channels, transcendentals=0, bytes_accessed=4 * positions * channels
        ),
        compiler_params=pltpu.CompilerParams(vmem_limit_bytes=16 << 20),
        name="opened",
    )(own, other, halo, band, vectors)
    entries = frames * tm * rows * height * COLS * (channels // GROUPS)
    head = pltpu.with_memory_space_constraint(later_weight[: 6 * channels], pltpu.VMEM)
    return second_part(rows, entries, sums, first, keep(opened), head, keep(conv_weight), vectors)


def solution(mesh):
    return jax.shard_map(
        shards,
        mesh=mesh,
        in_specs=(P(("tm", "height"), None), P(), P(), P(), P(), P(), P()),
        out_specs=P("tm", "height", None, None),
        check_vma=False,
    )
```
